256 devices in a mesh: chan: 128 (over z, x, y_hi, core), rng: 2 (over y_lo).
Axes of the slice: x: 4, y: 4 (y_hi: 2, y_lo: 2; y = y_hi * 2 + y_lo), z: 8, core: 2. Of those that a mesh axis runs over, the one named last changes fastest.
Arguments:
- radar_cube: bfloat16 [2, 4096, 64, 256], P(None, 'chan', None, 'rng'), may hold values from -31 to 31, as said below
- offsets: int32 [256], P('chan'), may hold values from 0 to 7
- train_index: int32 [128], P('rng'), may hold values from 0 to 127, as said below
- guard_mask: int32 [256], P('rng'), may hold values 0 or 1
- weights: bfloat16 [2, 256, 64, 96], P(None, 'chan'), may hold values from -0.625 to 0.625
Outputs:
- covariance: float32 [64, 256, 2, 9216], P('rng', 'chan')
- matched_stat: float32 [256, 64, 256], P('chan', None, 'rng')
- power_map: float32 [256, 64, 256], P('chan', None, 'rng')
The draws below stay inside these ranges and needn't reach their ends.
Inputs may be any that keep to these rules, and one draw needn't show every extreme that they name: `radar_cube`: samples are finite real numbers. `weights`: for every subarray and bin, at least one of the 96 complex weights is nonzero. `train_index`: each aligned block of 64 entries lists distinct gates of the matching block of 128 gates, counted from that block's first gate.
All inputs are finite; a program needn't handle non-finite values. No bound on the sum of `guard_mask` on one device may be relied on, other than what follows from the above.
Results may differ from the reference program's by a relative error of at most 0.0039.
Values may be sent and summed in bfloat16 or wider, within the bound.
A program may use at most 128 MiB of HBM per device.

```python
import math
from functools import partial
import jax
import jax.numpy as jnp
from jax import lax

PULSES = 64
CH_DEV = 32
SUB_LEN = 32
SUB_DEV = 2
SPAN = 8
RG_DEV = 128
STEP = 16
DOF = 96
TRAIN_DEV = 64
CHANNELS = 4096
NSUB = 256
GATES = 256
TRAIN = 128


def draw_radar_cube(key, part):
    first_key, second_key = jax.random.split(jax.random.fold_in(key, 11), 2)
    channel_pos = jnp.arange(CHANNELS, dtype=jnp.float32) / (CHANNELS - 1)
    rising = (3.0 ** channel_pos)[None, :, None, None]
    rough = jnp.exp(jax.random.uniform(second_key, (1, CHANNELS, 1, GATES), jnp.float32, -0.7, 0.7))
    base = jnp.clip(jax.random.normal(first_key, (2, CHANNELS, PULSES, GATES), jnp.float32), -4.0, 4.0)
    return (base * rising * rough).astype(jnp.bfloat16)


def draw_train_index(key, part):
    blocks = GATES // RG_DEV
    keys = jax.random.split(jax.random.fold_in(key, 23), blocks)
    chosen = jax.vmap(lambda each_key: jax.random.permutation(each_key, RG_DEV)[:TRAIN_DEV])(keys)
    return chosen.reshape(-1).astype(jnp.int32)


def touch_ends(drawn, rng, smallest, high):
    place = [jax.random.randint(jax.random.fold_in(rng, axis), (), 0, length) for axis, length in enumerate(drawn.shape)]
    widest = drawn.shape.index(max(drawn.shape))
    beside = place[:widest] + [(place[widest] + 1) % drawn.shape[widest]] + place[widest + 1:]
    return drawn.at[tuple(place)].set(smallest).at[tuple(beside)].set(high)


def levels(stream_key, dims, cuts, low, top_value):
    def one(axis_at, blocks):
        heights = jax.random.uniform(jax.random.fold_in(jax.random.fold_in(stream_key, 6), axis_at), (blocks,), jnp.float32, low / len(cuts), top_value / len(cuts))
        return jnp.repeat(jnp.exp(heights), dims[axis_at] // blocks).reshape((-1,) + (1,) * (len(dims) - axis_at - 1))

    factor_of = one(*cuts[0])
    for cut in cuts[1:]:
        factor_of = factor_of * one(*cut)
    return factor_of


def bell_draw(stream_key, dims, scale, bound, pieces=(), kind=jnp.bfloat16):
    entries = scale * jax.random.normal(stream_key, dims, jnp.float32)
    if pieces:
        entries = entries * levels(stream_key, dims, pieces, -0.22, 0.18)
    return jnp.clip(entries, -bound, bound).astype(kind)


def setup_inputs(seed: int = 0) -> dict:
    streams_of = jax.random.split(jax.random.key(seed), 6)
    radar_cube = draw_radar_cube(jax.random.fold_in(streams_of[5], 71), 0)
    offsets = touch_ends(jax.random.randint(streams_of[1], (NSUB,), 0, SPAN), jax.random.fold_in(streams_of[1], 1), 0, SPAN - 1).astype(jnp.int32)
    train_index = draw_train_index(jax.random.fold_in(streams_of[5], 71), 0)
    guard_mask = touch_ends((jax.random.randint(streams_of[3], (GATES,), 0, 4) < 3).astype(jnp.int32), jax.random.fold_in(streams_of[3], 1), 0, 1)
    weights = bell_draw(streams_of[4], (2, NSUB, PULSES, DOF), DOF ** -0.5, 0.625, ((1, 128),))
    return dict(radar_cube=radar_cube, offsets=offsets, train_index=train_index, guard_mask=guard_mask, weights=weights)


diag_load = 1.0
highest = lax.Precision.HIGHEST

def dft_table(pulses):
    freq = jnp.arange(pulses, dtype=jnp.int32)
    phase = freq[:, None] * freq[None, :] % pulses
    angle = phase.astype(jnp.float32) * (2.0 * math.pi / pulses)
    cosine = jnp.cos(angle) / math.sqrt(pulses)
    sine = jnp.sin(angle) / math.sqrt(pulses)
    upper = jnp.stack([cosine, sine], axis=1)
    lower = jnp.stack([-sine, cosine], axis=1)
    return jnp.stack([upper, lower], axis=0).astype(jnp.bfloat16)

def one_window(radar_cube, train_index, guard_mask, weights, dft_mat, item):
    subarray, window_offset = item
    first = subarray // SUB_DEV * CH_DEV + subarray % SUB_DEV * STEP + window_offset
    channels = ((first + jnp.arange(SUB_LEN, dtype=jnp.int32)) % CHANNELS).astype(jnp.int32)
    raw_pulses = jnp.take(radar_cube, channels, axis=1).astype(jnp.float32)
    spectra = jnp.einsum('yqxp,xmpr->ymqr', dft_mat.astype(jnp.float32), raw_pulses, precision=highest)
    spectra = lax.optimization_barrier(spectra.astype(jnp.bfloat16)).astype(jnp.float32)
    snapshots = jnp.stack([jnp.roll(spectra, 1 - shift_bin, axis=2) for shift_bin in range(3)], axis=1)
    snapshots = snapshots.reshape(2, DOF, PULSES, GATES)
    snap_real = snapshots[0]
    snap_imag = snapshots[1]
    chosen = lax.dynamic_index_in_dim(weights, subarray, axis=1, keepdims=False).astype(jnp.float32)
    weight_real = chosen[0]
    weight_imag = chosen[1]
    out_real = jnp.einsum('kd,dkr->kr', weight_real, snap_real, precision=highest) + jnp.einsum('kd,dkr->kr', weight_imag, snap_imag, precision=highest)
    out_imag = jnp.einsum('kd,dkr->kr', weight_real, snap_imag, precision=highest) - jnp.einsum('kd,dkr->kr', weight_imag, snap_real, precision=highest)
    out_power = out_real * out_real + out_imag * out_imag
    gates = (jnp.arange(TRAIN, dtype=jnp.int32) // TRAIN_DEV * RG_DEV + train_index).astype(jnp.int32)
    keep = jnp.take(guard_mask, gates).astype(jnp.float32)
    picked = jnp.take(snapshots, gates, axis=3) * keep
    pick_real = picked[0]
    pick_imag = picked[1]
    cov_real = (jnp.einsum('ikt,jkt->kij', pick_real, pick_real, precision=highest) + jnp.einsum('ikt,jkt->kij', pick_imag, pick_imag, precision=highest)) / TRAIN
    cov_imag = (jnp.einsum('ikt,jkt->kij', pick_imag, pick_real, precision=highest) - jnp.einsum('ikt,jkt->kij', pick_real, pick_imag, precision=highest)) / TRAIN
    prod_real = jnp.einsum('kij,kj->ki', cov_real, weight_real, precision=highest) - jnp.einsum('kij,kj->ki', cov_imag, weight_imag, precision=highest)
    prod_imag = jnp.einsum('kij,kj->ki', cov_real, weight_imag, precision=highest) + jnp.einsum('kij,kj->ki', cov_imag, weight_real, precision=highest)
    quad_form = lax.optimization_barrier(jnp.sum(weight_real * prod_real + weight_imag * prod_imag, axis=-1)) + diag_load * lax.optimization_barrier(jnp.sum(weight_real * weight_real + weight_imag * weight_imag, axis=-1))
    matched = out_power / quad_form[:, None]
    covariance = jnp.stack([cov_real, cov_imag], axis=1).reshape(PULSES, 2, DOF * DOF)
    return (covariance, matched, out_power)

def reference(radar_cube, offsets, train_index, guard_mask, weights):
    dft_mat = dft_table(PULSES)
    items = (jnp.arange(NSUB, dtype=jnp.int32), offsets.astype(jnp.int32))
    covs, matched_stat, out_power = lax.map(partial(one_window, radar_cube, train_index, guard_mask, weights, dft_mat), items)
    covariance = jnp.transpose(covs, (1, 0, 2, 3))
    total_power = jnp.sum(out_power)
    mean_power = total_power / (NSUB * PULSES * GATES)
    power_map = out_power / (mean_power + 1e-06)
    return (covariance, matched_stat, power_map)
```

```python
import functools
import math

import jax
import jax.numpy as jnp
import numpy as np
from jax import lax
from jax.experimental import pallas as pl
from jax.experimental.pallas import tpu as pltpu
from jax.sharding import PartitionSpec as P

MESH = pl.DeviceIdType.MESH
F32 = jnp.float32
BF16 = jnp.bfloat16

PULSES = 64
CH = 32
SUB = 32
HALO = 24
EXT = CH + HALO
GATES = 128
TRAIN = 64
HALF = 32
BINS = HALF + 2
SLOTS = PULSES + 2
GROUP = 6
CHUNK = 4
N_CHUNK = HALF // CHUNK
ROWS = 144


def dft_matrix():
    freq = np.arange(PULSES)
    angle = (freq[:, None] * freq[None, :] % PULSES) * (2.0 * math.pi / PULSES)
    cosine = np.cos(angle) / math.sqrt(PULSES)
    sine = np.sin(angle) / math.sqrt(PULSES)
    return np.block([[cosine, sine], [-sine, cosine]]).astype(jnp.bfloat16)


def dot(a, b):
    return jnp.dot(a, b, preferred_element_type=F32)


def dot_nt(a, b):
    return lax.dot_general(a, b, (((1,), (1,)), ((), ())), preferred_element_type=F32)


def turned_by(x, shift):
    return pltpu.roll(x, shift % x.shape[0], 0) if shift else x


def kernel(
    sizes,
    off_ref,
    cube_hbm,
    idx_ref,
    guard_ref,
    wts_ref,
    dft_ref,
    cov_hbm,
    matched_ref,
    pmap_ref,
    cube,
    spec,
    bins_a,
    bins_b,
    train,
    train_halo,
    got_train,
    got_halo,
    send_wts,
    got_wts,
    lhs,
    filt_re,
    filt_im,
    send_part,
    got_part,
    send_quad,
    got_quad,
    sum_a,
    sum_b,
    ext_a,
    ext_b,
    rhs_re,
    rhs_im,
    lhs_cov,
    cov,
    cube_sem,
    cov_sem,
    send_sem,
    recv_sem,
    a_send,
    a_recv,
    b_send,
    b_recv,
):
    n_z, n_xy, n_chan, n_rng = sizes
    n_a, n_b = n_xy * n_rng, n_z * 2
    chan, rng = lax.axis_index("chan"), lax.axis_index("rng")
    other = 1 - rng
    prev, following = lax.rem(chan + n_chan - 1, n_chan), lax.rem(chan + 1, n_chan)
    core = lax.rem(chan, 2)
    chip = chan // 2
    z, xy = chip // n_xy, lax.rem(chip, n_xy)
    my_a, my_b = xy * n_rng + rng, z * 2 + core

    def peer_a(step):
        slot = lax.rem(my_a + step, n_a)
        return slot, ((z * n_xy + slot // n_rng) * 2 + core, lax.rem(slot, n_rng))

    def peer_b(step):
        slot = lax.rem(my_b + step, n_b)
        return slot, (((slot // 2) * n_xy + xy) * 2 + lax.rem(slot, 2), rng)

    def remote(src, dst, k, device):
        return pltpu.make_async_remote_copy(
            src_ref=src,
            dst_ref=dst,
            send_sem=send_sem.at[k],
            recv_sem=recv_sem.at[k],
            device_id=device,
            device_id_type=MESH,
        )

    fetch = pltpu.make_async_copy(cube_hbm, cube, cube_sem)
    fetch.start()
    barrier = pltpu.get_barrier_semaphore()
    for device in ((prev, rng), (following, rng), (prev, other), (following, other)):
        pl.semaphore_signal(barrier, inc=1, device_id=device, device_id_type=MESH)

    def greet_a(step, carry):
        pl.semaphore_signal(barrier, inc=1, device_id=peer_a(step)[1], device_id_type=MESH)
        return carry

    def greet_b(step, carry):
        pl.semaphore_signal(barrier, inc=1, device_id=peer_b(step)[1], device_id_type=MESH)
        return carry

    lax.fori_loop(1, n_a, greet_a, 0)
    lax.fori_loop(1, n_b, greet_b, 0)

    lane = lax.broadcasted_iota(jnp.int32, (1, 128), 1)
    depth = lax.broadcasted_iota(jnp.int32, (96, 128), 0)
    placed = [[jnp.zeros((PULSES, 128), F32) for _ in range(3)] for _ in range(2)]
    for sub in range(2):
        for part in range(2):
            value = wts_ref[part, sub]
            for ahead in range(2):
                at = lax.rem(lane, 32) + (32 * ahead - 16 * sub) - off_ref[sub]
                fits = (at >= 0) & (at < SUB) & (lane // 32 == sub * 2 + part)
                for b in range(3):
                    hot = jnp.where(depth == jnp.where(fits, at + b * SUB, -1), 1.0, 0.0).astype(BF16)
                    placed[ahead][b] = placed[ahead][b] + dot(value, hot)
    for b in range(3):
        send_wts[b] = turned_by(placed[1][b], b - 1).astype(BF16)

    def fill_lhs(tables):
        for b in range(3):
            lhs[pl.ds(b * 2, PULSES, stride=8), :] = tables[b]
            lhs[pl.ds(b * 2 + 1, PULSES, stride=8), :] = pltpu.roll(tables[b], 64, 1)

    gate = lax.broadcasted_iota(jnp.int32, (GATES, 128), 0)
    wanted = jnp.concatenate([idx_ref[...], idx_ref[...]], axis=1)
    hits = jnp.where(gate == wanted, 1.0, 0.0)
    guard = jnp.broadcast_to(guard_ref[...].astype(F32), (8, GATES)).astype(BF16)
    keep = dot(guard, hits.astype(BF16))[0:1]
    pick = (hits * keep).astype(BF16)
    counts = dot_nt(jnp.full((8, 128), 0.5, BF16), pick)[0:1]

    pl.semaphore_wait(barrier, 4 + (n_a - 1) + (n_b - 1))
    wts_copy = remote(send_wts, got_wts, 0, (following, rng))
    wts_copy.start()
    fill_lhs([turned_by(placed[0][b], b - 1) for b in range(3)])

    fetch.wait()
    table = dft_ref[...]

    def doppler(step, carry):
        for u in range(2):
            m = step * 4 + 2 * u
            pair = [jnp.concatenate([cube[0, m + v], cube[1, m + v]], axis=0) for v in range(2)]
            out = dot(table, jnp.concatenate(pair, axis=1))
            for v in range(2):
                for part in range(2):
                    start = pl.multiple_of((part * CH + m + v) * PULSES, PULSES)
                    spec[pl.ds(start, PULSES), :] = out[part * 64 : part * 64 + 64, v * 128 : v * 128 + 128]
        return carry

    lax.fori_loop(0, CH // 4, doppler, 0)

    left = lax.broadcasted_iota(jnp.int32, (CH, 128), 1) < TRAIN

    def per_bin(step, carry):
        rows = []
        for u in range(GROUP):
            k = lax.rem(step * GROUP + u + PULSES - 1, PULSES)
            re = spec[pl.ds(k, CH, stride=PULSES), :]
            im = spec[pl.ds(k + CH * PULSES, CH, stride=PULSES), :]
            both = jnp.concatenate([re, im], axis=0).astype(BF16)
            bins_a[k] = both
            bins_b[k] = jnp.concatenate([im, -re], axis=0).astype(BF16)
            rows.append(both)
        chosen = dot(jnp.concatenate(rows, axis=0), pick)
        tiles = []
        for u in range(GROUP):
            tile = jnp.where(left, chosen[u * 64 : u * 64 + 32], chosen[u * 64 + 32 : u * 64 + 64])
            train[step * GROUP + u] = tile.astype(BF16)
            tiles.append(tile[:HALO])
        start = pl.multiple_of(step * (GROUP * HALO), GROUP * HALO)
        train_halo[pl.ds(start, GROUP * HALO), :] = jnp.concatenate(tiles, axis=0).astype(BF16)
        return carry

    lax.fori_loop(0, SLOTS // GROUP, per_bin, 0)

    halo_rows = BINS * HALO
    train_copy = remote(train.at[pl.ds(other * HALF, BINS)], got_train, 1, (chan, other))
    same_copy = remote(
        train_halo.at[pl.ds(pl.multiple_of(rng * (HALF * HALO), HALF * HALO), halo_rows)], got_halo.at[0], 2, (prev, rng)
    )
    cross_copy = remote(
        train_halo.at[pl.ds(pl.multiple_of(other * (HALF * HALO), HALF * HALO), halo_rows)], got_halo.at[1], 3, (prev, other)
    )
    train_copy.start()
    same_copy.start()
    cross_copy.start()

    def filtered():
        def one(step, carry):
            for u in range(8):
                k = step * 8 + u
                row = pl.multiple_of(k * 8, 8)
                weight = lhs[pl.ds(row, 8), :][:, :64].astype(BF16)
                out = dot(weight, jnp.concatenate([bins_a[k], bins_b[k]], axis=1))
                filt_re[pl.ds(row, 8), :] = out[:, :128]
                filt_im[pl.ds(row, 8), :] = out[:, 128:]
            return carry

        lax.fori_loop(0, PULSES // 8, one, 0)
        sums = []
        for sub in range(2):
            for ref in (filt_re, filt_im):
                terms = [turned_by(ref[pl.ds(b * 2 + sub, PULSES, stride=8), :], 1 - b) for b in range(3)]
                sums.append(terms[0] + terms[1] + terms[2])
        return sums

    own = filtered()
    wts_copy.wait()
    fill_lhs([got_wts[b].astype(F32) for b in range(3)])
    for part, value in enumerate(filtered()):
        send_part[part] = value
    part_copy = remote(send_part, got_part, 4, (prev, rng))
    part_copy.start()

    norms = []
    for sub in range(2):
        re, im = wts_ref[0, sub].astype(F32), wts_ref[1, sub].astype(F32)
        norms.append(jnp.sum(re * re + im * im, axis=1, keepdims=True))

    def own_rows(k, carry):
        start = pl.multiple_of(k * EXT, 8)
        ext_a[pl.ds(start, CH), :] = train[rng * HALF + k].astype(F32)
        return carry

    lax.fori_loop(0, BINS, own_rows, 0)

    part_copy.wait()
    powers = []
    for sub in range(2):
        re = own[2 * sub] + got_part[2 * sub]
        im = own[2 * sub + 1] + got_part[2 * sub + 1]
        powers.append(re * re + im * im)
    quads = [jnp.sum(p * counts, axis=1, keepdims=True) for p in powers]
    send_quad[...] = jnp.where(lane < 64, quads[0], quads[1])
    quad_copy = remote(send_quad, got_quad, 5, (chan, other))
    quad_copy.start()
    sum_a[my_a] = jnp.sum(powers[0] + powers[1], axis=0, keepdims=True)

    def copy_a(step):
        return pltpu.make_async_remote_copy(
            src_ref=sum_a.at[my_a],
            dst_ref=sum_a.at[my_a],
            send_sem=a_send.at[step],
            recv_sem=a_recv.at[my_a],
            device_id=peer_a(step)[1],
            device_id_type=MESH,
        )

    def copy_b(step):
        return pltpu.make_async_remote_copy(
            src_ref=sum_b.at[my_b],
            dst_ref=sum_b.at[my_b],
            send_sem=b_send.at[step],
            recv_sem=b_recv.at[my_b],
            device_id=peer_b(step)[1],
            device_id_type=MESH,
        )

    def start_a(step, carry):
        copy_a(step).start()
        return carry

    def start_b(step, carry):
        copy_b(step).start()
        return carry

    def finish_a(step, carry):
        slot, device = peer_a(step)
        pltpu.make_async_remote_copy(
            src_ref=sum_a.at[my_a],
            dst_ref=sum_a.at[slot],
            send_sem=a_send.at[step],
            recv_sem=a_recv.at[slot],
            device_id=device,
            device_id_type=MESH,
        ).wait()
        return carry

    def finish_b(step, carry):
        slot, device = peer_b(step)
        pltpu.make_async_remote_copy(
            src_ref=sum_b.at[my_b],
            dst_ref=sum_b.at[slot],
            send_sem=b_send.at[step],
            recv_sem=b_recv.at[slot],
            device_id=device,
            device_id_type=MESH,
        ).wait()
        return carry

    lax.fori_loop(1, n_a, start_a, 0)

    train_copy.wait()
    same_copy.wait()
    cross_copy.wait()
    low = lax.broadcasted_iota(jnp.int32, (SUB, 128), 1) < TRAIN

    def windows(k, carry):
        start = pl.multiple_of(k * EXT, 8)
        ext_b[pl.ds(start, CH), :] = got_train[k].astype(F32)
        return carry

    lax.fori_loop(0, BINS, windows, 0)

    def halos(step, carry):
        rows = pl.multiple_of(step * (2 * HALO), 2 * HALO)
        for ext, which in ((ext_a, 0), (ext_b, 1)):
            pair = got_halo[which, pl.ds(rows, 2 * HALO), :].astype(F32)
            for u in range(2):
                start = pl.multiple_of((step * 2 + u) * EXT + CH, 8)
                ext[pl.ds(start, HALO), :] = pair[u * HALO : u * HALO + HALO]
        return carry

    lax.fori_loop(0, BINS // 2, halos, 0)

    def arrange(k, carry):
        row = pl.multiple_of(k * SUB, SUB)
        for sub in range(2):
            start = k * EXT + 16 * sub + off_ref[sub]
            natural = [ext[pl.ds(start, SUB), :] for ext in (ext_a, ext_b)]
            turned = [pltpu.roll(x, 64, 1) for x in natural]
            rhs_re[sub, pl.ds(row, SUB), :] = jnp.concatenate(natural, axis=1).astype(BF16)
            rhs_im[sub, pl.ds(row, SUB), :] = jnp.concatenate([jnp.where(low, -x, x) for x in turned], axis=1).astype(BF16)
            by_four = [
                jnp.concatenate([ext[pl.ds(start + a, 8, stride=4), :] for a in range(4)], axis=0)
                for ext in (ext_a, ext_b)
            ]
            lhs_cov[sub, pl.ds(row, SUB), :] = jnp.concatenate(by_four, axis=1).astype(BF16)
        return carry

    lax.fori_loop(0, BINS, arrange, 0)

    col = lax.broadcasted_iota(jnp.int32, (24, 128), 1)

    def one_bin(k, carry):
        row = pl.multiple_of(k * SUB, SUB)
        for sub in range(2):
            left_rows = lhs_cov[sub, pl.ds(row, 96), :]
            right = jnp.concatenate([rhs_re[sub, pl.ds(row, 128), :], rhs_im[sub, pl.ds(row, 128), :]], axis=0)
            out = dot_nt(left_rows, right) * (1.0 / 128.0)
            base = (k * 2 + sub) * ROWS
            for part in range(2):
                half = out[:, part * 128 : part * 128 + 128]
                by = [
                    jnp.concatenate([half[b * 32 + a * 8 : b * 32 + a * 8 + 8] for b in range(3)], axis=0)
                    for a in range(4)
                ]
                r1, r2, r3 = pltpu.roll(by[1], 96, 1), pltpu.roll(by[2], 64, 1), pltpu.roll(by[3], 32, 1)
                cov[pl.ds(base + part, 24, stride=6), :] = jnp.where(col < 96, by[0], r1)
                cov[pl.ds(base + 2 + part, 24, stride=6), :] = jnp.where(col < 64, r1, r2)
                cov[pl.ds(base + 4 + part, 24, stride=6), :] = jnp.where(col < 32, r2, r3)
        return carry

    def cov_copy(chunk):
        rows = pl.ds(pl.multiple_of(chunk * (CHUNK * 2 * ROWS), CHUNK * 2 * ROWS), CHUNK * 2 * ROWS)
        return pltpu.make_async_copy(cov.at[rows], cov_hbm.at[rows], cov_sem.at[chunk])

    def one_chunk(chunk, carry):
        lax.fori_loop(chunk * CHUNK, chunk * CHUNK + CHUNK, one_bin, 0)
        cov_copy(chunk).start()
        return carry

    def chunk_done(chunk, carry):
        cov_copy(chunk).wait()
        return carry

    lax.fori_loop(0, N_CHUNK // 2, one_chunk, 0)

    lax.fori_loop(1, n_a, finish_a, 0)
    sum_b[my_b] = jnp.sum(sum_a[...], axis=0)
    lax.fori_loop(1, n_b, start_b, 0)
    lax.fori_loop(N_CHUNK // 2, N_CHUNK, one_chunk, 0)

    quad_copy.wait()
    quad_sum = send_quad[...] + got_quad[...]
    for sub in range(2):
        quad = quad_sum[:, sub * 64 : sub * 64 + 1] * (1.0 / 128.0) + norms[sub]
        matched_ref[sub] = powers[sub] / quad

    lax.fori_loop(1, n_b, finish_b, 0)
    total = jnp.sum(jnp.sum(sum_b[...], axis=0), axis=1, keepdims=True)
    mean = total * (1.0 / (n_chan * n_rng * 2 * PULSES * GATES)) + 1e-6
    for sub in range(2):
        pmap_ref[sub] = powers[sub] / mean
    lax.fori_loop(0, N_CHUNK, chunk_done, 0)


def local(sizes, radar_cube, offsets, train_index, guard_mask, weights):
    n_z, n_xy, n_chan, n_rng = sizes
    n_a, n_b = n_xy * n_rng, n_z * 2
    dma = pltpu.SemaphoreType.DMA
    vmem = pl.BlockSpec(memory_space=pltpu.VMEM)
    rows = HALF * 2 * ROWS
    cov, matched, pmap = pl.pallas_call(
        functools.partial(kernel, sizes),
        out_shape=(
            jax.ShapeDtypeStruct((rows, 128), F32),
            jax.ShapeDtypeStruct((2, PULSES, GATES), F32),
            jax.ShapeDtypeStruct((2, PULSES, GATES), F32),
        ),
        in_specs=[
            pl.BlockSpec(memory_space=pltpu.SMEM),
            pl.BlockSpec(memory_space=pl.ANY),
            vmem,
            vmem,
            vmem,
            vmem,
        ],
        out_specs=(pl.BlockSpec(memory_space=pl.ANY), vmem, vmem),
        scratch_shapes=[
            pltpu.VMEM((2, CH, PULSES, GATES), BF16),
            pltpu.VMEM((2 * CH * PULSES, GATES), F32),
            pltpu.VMEM((PULSES, 2 * CH, GATES), BF16),
            pltpu.VMEM((PULSES, 2 * CH, GATES), BF16),
            pltpu.VMEM((SLOTS, CH, 128), BF16),
            pltpu.VMEM((SLOTS * HALO, 128), BF16),
            pltpu.VMEM((BINS, CH, 128), BF16),
            pltpu.VMEM((2, BINS * HALO, 128), BF16),
            pltpu.VMEM((3, PULSES, 128), BF16),
            pltpu.VMEM((3, PULSES, 128), BF16),
            pltpu.VMEM((PULSES * 8, 128), F32),
            pltpu.VMEM((PULSES * 8, 128), F32),
            pltpu.VMEM((PULSES * 8, 128), F32),
            pltpu.VMEM((4, PULSES, GATES), F32),
            pltpu.VMEM((4, PULSES, GATES), F32),
            pltpu.VMEM((PULSES, 128), F32),
            pltpu.VMEM((PULSES, 128), F32),
            pltpu.VMEM((n_a, 1, 128), F32),
            pltpu.VMEM((n_b, 1, 128), F32),
            pltpu.VMEM((BINS * EXT, 128), F32),
            pltpu.VMEM((BINS * EXT, 128), F32),
            pltpu.VMEM((2, (BINS + 1) * SUB, 256), BF16),
            pltpu.VMEM((2, (BINS + 1) * SUB, 256), BF16),
            pltpu.VMEM((2, (BINS + 1) * SUB, 256), BF16),
            pltpu.VMEM((rows, 128), F32),
            dma,
            dma((N_CHUNK,)),
            dma((6,)),
            dma((6,)),
            dma((n_a,)),
            dma((n_a,)),
            dma((n_b,)),
            dma((n_b,)),
        ],
        compiler_params=pltpu.CompilerParams(collective_id=0, has_side_effects=True),
    )(
        offsets,
        radar_cube,
        train_index.reshape(1, -1),
        guard_mask.reshape(1, -1),
        weights,
        jnp.asarray(dft_matrix()),
    )
    cov = cov.reshape(HALF, 2, ROWS // 2, 2, 128).transpose(0, 1, 3, 2, 4).reshape(HALF, 2, 2, ROWS * 64)
    return cov, matched, pmap


def solution(mesh):
    n_chan, n_rng = mesh.shape["chan"], mesh.shape["rng"]
    n_xy = 8 if n_chan >= 64 else 2
    sizes = (n_chan // (2 * n_xy), n_xy, n_chan, n_rng)
    return jax.shard_map(
        functools.partial(local, sizes),
        mesh=mesh,
        in_specs=(
            P(None, "chan", None, "rng"),
            P("chan"),
            P("rng"),
            P("rng"),
            P(None, "chan", None, None),
        ),
        out_specs=(P("rng", "chan", None, None), P("chan", None, "rng"), P("chan", None, "rng")),
        check_vma=False,
    )
```

```python
import functools
import math

import jax
import jax.numpy as jnp
import numpy as np
from jax import lax
from jax.experimental import pallas as pl
from jax.experimental.pallas import tpu as pltpu
from jax.sharding import PartitionSpec as P

MESH = pl.DeviceIdType.MESH
F32 = jnp.float32
BF16 = jnp.bfloat16

PULSES = 64
CH = 32
SUB = 32
HALO = 24
EXT = CH + HALO
GATES = 128
TRAIN = 64
HALF = 32
BINS = HALF + 2
SLOTS = PULSES + 2
GROUP = 6
ROWS = 144
PITCH = PULSES + 8
PIECES = ((0, 10), (10, 8), (18, 8), (26, 8))


def dft_matrix():
    freq = np.arange(PULSES)
    angle = (freq[:, None] * freq[None, :] % PULSES) * (2.0 * math.pi / PULSES)
    cosine = np.cos(angle) / math.sqrt(PULSES)
    sine = np.sin(angle) / math.sqrt(PULSES)
    return np.block([[cosine, sine], [-sine, cosine]]).astype(jnp.bfloat16)


def dot(a, b):
    return jnp.dot(a, b, preferred_element_type=F32)


def dot_nt(a, b):
    return lax.dot_general(a, b, (((1,), (1,)), ((), ())), preferred_element_type=F32)


def turned_by(x, shift):
    return pltpu.roll(x, shift % x.shape[0], 0) if shift else x


def kernel(
    sizes,
    off_hbm,
    cube_hbm,
    idx_hbm,
    guard_hbm,
    wts_hbm,
    dft_hbm,
    cov,
    matched_ref,
    pmap_ref,
    off_ref,
    cube,
    idx_ref,
    guard_ref,
    wts_ref,
    dft_ref,
    spec,
    bins_a,
    bins_b,
    train,
    train_halo,
    got_train,
    got_same,
    got_cross,
    send_wts,
    got_wts,
    lhs,
    filt_re,
    filt_im,
    send_part,
    got_part,
    send_quad,
    got_quad,
    sum_a,
    sum_b,
    ext_a,
    ext_b,
    rhs_re,
    rhs_im,
    lhs_cov,
    tiles,
    fetch_sem,
    send_sem,
    recv_sem,
    train_send,
    train_recv,
    same_send,
    same_recv,
    cross_send,
    cross_recv,
    a_send,
    a_recv,
    b_send,
    b_recv,
):
    n_z, n_xy, n_chan, n_rng = sizes
    n_a, n_b = n_xy * n_rng, n_z * 2
    chan, rng = lax.axis_index("chan"), lax.axis_index("rng")
    other = 1 - rng
    prev, following = lax.rem(chan + n_chan - 1, n_chan), lax.rem(chan + 1, n_chan)
    core = lax.rem(chan, 2)
    chip = chan // 2
    z, xy = chip // n_xy, lax.rem(chip, n_xy)
    my_a, my_b = xy * n_rng + rng, z * 2 + core

    def peer_a(step):
        slot = lax.rem(my_a + step, n_a)
        return slot, ((z * n_xy + slot // n_rng) * 2 + core, lax.rem(slot, n_rng))

    def peer_b(step):
        slot = lax.rem(my_b + step, n_b)
        return slot, (((slot // 2) * n_xy + xy) * 2 + lax.rem(slot, 2), rng)

    def remote(src, dst, send, recv, device):
        return pltpu.make_async_remote_copy(
            src_ref=src,
            dst_ref=dst,
            send_sem=send,
            recv_sem=recv,
            device_id=device,
            device_id_type=MESH,
        )

    fetches = [
        pltpu.make_async_copy(src, dst, fetch_sem.at[i])
        for i, (src, dst) in enumerate(
            (
                (off_hbm, off_ref),
                (wts_hbm, wts_ref),
                (idx_hbm, idx_ref),
                (guard_hbm, guard_ref),
                (dft_hbm, dft_ref),
                (cube_hbm, cube),
            )
        )
    ]
    for fetch in fetches:
        fetch.start()
    barrier = pltpu.get_barrier_semaphore()
    for device in ((prev, rng), (following, rng), (prev, other), (following, other)):
        pl.semaphore_signal(barrier, inc=1, device_id=device, device_id_type=MESH)

    def greet_a(step, carry):
        pl.semaphore_signal(barrier, inc=1, device_id=peer_a(step)[1], device_id_type=MESH)
        return carry

    def greet_b(step, carry):
        pl.semaphore_signal(barrier, inc=1, device_id=peer_b(step)[1], device_id_type=MESH)
        return carry

    lax.fori_loop(1, n_a, greet_a, 0)
    lax.fori_loop(1, n_b, greet_b, 0)

    fetches[0].wait()
    fetches[1].wait()
    lane = lax.broadcasted_iota(jnp.int32, (1, 128), 1)
    depth = lax.broadcasted_iota(jnp.int32, (96, 128), 0)
    placed = [[jnp.zeros((PULSES, 128), F32) for _ in range(3)] for _ in range(2)]
    for sub in range(2):
        for part in range(2):
            value = wts_ref[part, sub]
            for ahead in range(2):
                at = lax.rem(lane, 32) + (32 * ahead - 16 * sub) - off_ref[sub]
                fits = (at >= 0) & (at < SUB) & (lane // 32 == sub * 2 + part)
                for b in range(3):
                    hot = jnp.where(depth == jnp.where(fits, at + b * SUB, -1), 1.0, 0.0).astype(BF16)
                    placed[ahead][b] = placed[ahead][b] + dot(value, hot)
    for b in range(3):
        send_wts[b] = turned_by(placed[1][b], b - 1).astype(BF16)

    def fill_lhs(tables):
        for b in range(3):
            lhs[pl.ds(b * 2, PULSES, stride=8), :] = tables[b]
            lhs[pl.ds(b * 2 + 1, PULSES, stride=8), :] = pltpu.roll(tables[b], 64, 1)

    fetches[2].wait()
    fetches[3].wait()
    gate = lax.broadcasted_iota(jnp.int32, (GATES, 128), 0)
    wanted = jnp.concatenate([idx_ref[...], idx_ref[...]], axis=1)
    hits = jnp.where(gate == wanted, 1.0, 0.0)
    guard = jnp.broadcast_to(guard_ref[...].astype(F32), (8, GATES)).astype(BF16)
    keep = dot(guard, hits.astype(BF16))[0:1]
    pick = (hits * keep).astype(BF16)
    counts = dot_nt(jnp.full((8, 128), 0.5, BF16), pick)[0:1]

    pl.semaphore_wait(barrier, 4 + (n_a - 1) + (n_b - 1))
    wts_copy = remote(send_wts, got_wts, send_sem.at[0], recv_sem.at[0], (following, rng))
    wts_copy.start()

    fetches[4].wait()
    fetches[5].wait()
    table = dft_ref[...]

    def doppler(step, carry):
        for u in range(4):
            m = step * 8 + 2 * u
            pair = [jnp.concatenate([cube[0, m + v], cube[1, m + v]], axis=0) for v in range(2)]
            out = dot(table, jnp.concatenate(pair, axis=1))
            for v in range(2):
                for part in range(2):
                    start = pl.multiple_of((part * CH + m + v) * PITCH, 8)
                    spec[pl.ds(start, PULSES), :] = out[part * 64 : part * 64 + 64, v * 128 : v * 128 + 128]
        return carry

    lax.fori_loop(0, CH // 8, doppler, 0)

    left = lax.broadcasted_iota(jnp.int32, (CH, 128), 1) < TRAIN

    def gather_bins(step):
        for u in range(GROUP):
            k = lax.rem(step * GROUP + u + PULSES - 1, PULSES)
            re = spec[pl.ds(k, CH, stride=PITCH), :]
            im = spec[pl.ds(k + CH * PITCH, CH, stride=PITCH), :]
            bins_a[k] = jnp.concatenate([re, im], axis=0).astype(BF16)
            bins_b[k] = jnp.concatenate([im, -re], axis=0).astype(BF16)

    def choose_gates(step):
        rows = [bins_a[lax.rem(step * GROUP + u + PULSES - 1, PULSES)] for u in range(GROUP)]
        chosen = dot(jnp.concatenate(rows, axis=0), pick)
        halo = []
        for u in range(GROUP):
            tile = jnp.where(left, chosen[u * 64 : u * 64 + 32], chosen[u * 64 + 32 : u * 64 + 64])
            train[step * GROUP + u] = tile.astype(BF16)
            halo.append(tile[:HALO])
        start = pl.multiple_of(step * (GROUP * HALO), GROUP * HALO)
        train_halo[pl.ds(start, GROUP * HALO), :] = jnp.concatenate(halo, axis=0).astype(BF16)

    def per_bin(step, carry):
        choose_gates(step - 1)
        gather_bins(step)
        return carry

    gather_bins(0)
    lax.fori_loop(1, SLOTS // GROUP, per_bin, 0)
    choose_gates(SLOTS // GROUP - 1)

    def train_copy(piece):
        first, count = PIECES[piece]
        return remote(
            train.at[pl.ds(other * HALF + first, count)],
            got_train.at[pl.ds(first, count)],
            train_send.at[piece],
            train_recv.at[piece],
            (chan, other),
        )

    def same_copy(piece):
        first, count = PIECES[piece]
        start = pl.multiple_of(rng * (HALF * HALO) + first * HALO, 16)
        return remote(
            train_halo.at[pl.ds(start, count * HALO)],
            got_same.at[pl.ds(first * HALO, count * HALO)],
            same_send.at[piece],
            same_recv.at[piece],
            (prev, rng),
        )

    def cross_copy(piece):
        first, count = PIECES[piece]
        return remote(
            train.at[pl.ds(other * HALF + first, count)],
            got_cross.at[pl.ds(first, count)],
            cross_send.at[piece],
            cross_recv.at[piece],
            (prev, other),
        )

    def relay_copy(piece):
        first, count = PIECES[piece]
        return remote(
            got_train.at[pl.ds(first, count)],
            got_cross.at[pl.ds(first, count)],
            cross_send.at[piece],
            cross_recv.at[piece],
            (prev, rng),
        )

    train_copy(0).start()

    def filtered():
        def one(step, carry):
            for u in range(16):
                k = step * 16 + u
                row = pl.multiple_of(k * 8, 8)
                weight = lhs[pl.ds(row, 8), :][:, :64].astype(BF16)
                out = dot(weight, jnp.concatenate([bins_a[k], bins_b[k]], axis=1))
                filt_re[pl.ds(row, 8), :] = out[:, :128]
                filt_im[pl.ds(row, 8), :] = out[:, 128:]
            return carry

        lax.fori_loop(0, PULSES // 16, one, 0)
        sums = []
        for sub in range(2):
            for ref in (filt_re, filt_im):
                terms = [turned_by(ref[pl.ds(b * 2 + sub, PULSES, stride=8), :], 1 - b) for b in range(3)]
                sums.append(terms[0] + terms[1] + terms[2])
        return sums

    wts_copy.wait()
    fill_lhs([got_wts[b].astype(F32) for b in range(3)])
    for part, value in enumerate(filtered()):
        send_part[part] = value
    part_copy = remote(send_part, got_part, send_sem.at[1], recv_sem.at[1], (prev, rng))
    part_copy.start()
    for piece in range(len(PIECES)):
        if piece:
            train_copy(piece).start()
        same_copy(piece).start()

        @pl.when(core == 0)
        def _(piece=piece):
            cross_copy(piece).start()

    fill_lhs([turned_by(placed[0][b], b - 1) for b in range(3)])
    own = filtered()

    norms = []
    for sub in range(2):
        re, im = wts_ref[0, sub].astype(F32), wts_ref[1, sub].astype(F32)
        norms.append(jnp.sum(re * re + im * im, axis=1, keepdims=True))

    part_copy.wait()
    powers = []
    for sub in range(2):
        re = own[2 * sub] + got_part[2 * sub]
        im = own[2 * sub + 1] + got_part[2 * sub + 1]
        powers.append(re * re + im * im)
    sum_b[my_b] = jnp.sum(powers[0] + powers[1], axis=0, keepdims=True)

    def start_a(step, carry):
        device = peer_a(step)[1]
        remote(sum_a.at[my_a], sum_a.at[my_a], a_send.at[step], a_recv.at[my_a], device).start()
        return carry

    def start_b(step, carry):
        device = peer_b(step)[1]
        remote(sum_b.at[my_b], sum_b.at[my_b], b_send.at[step], b_recv.at[my_b], device).start()
        return carry

    def finish_a(step, carry):
        slot, device = peer_a(step)
        remote(sum_a.at[my_a], sum_a.at[slot], a_send.at[step], a_recv.at[slot], device).wait()
        return carry

    def finish_b(step, carry):
        slot, device = peer_b(step)
        remote(sum_b.at[my_b], sum_b.at[slot], b_send.at[step], b_recv.at[slot], device).wait()
        return carry

    lax.fori_loop(1, n_b, start_b, 0)
    quads = [jnp.sum(p * counts, axis=1, keepdims=True) for p in powers]
    send_quad[...] = jnp.where(lane < 64, quads[0], quads[1])
    quad_copy = remote(send_quad, got_quad, send_sem.at[2], recv_sem.at[2], (chan, other))
    quad_copy.start()

    low = lax.broadcasted_iota(jnp.int32, (SUB, 128), 1) < TRAIN

    def arrange(step, carry):
        rows = pl.multiple_of(step * (2 * HALO), 2 * HALO)
        same = got_same[pl.ds(rows, 2 * HALO), :].astype(F32)
        for u in range(2):
            k = step * 2 + u
            start = pl.multiple_of(k * EXT, 8)
            ext_a[pl.ds(start, CH), :] = train[rng * HALF + k].astype(F32)
            ext_a[pl.ds(start + CH, HALO), :] = same[u * HALO : u * HALO + HALO]
            ext_b[pl.ds(start, CH), :] = got_train[k].astype(F32)
            ext_b[pl.ds(start + CH, HALO), :] = got_cross[k].astype(F32)[:HALO]
        for u in range(2):
            k = step * 2 + u
            row = pl.multiple_of(k * SUB, SUB)
            for sub in range(2):
                start = k * EXT + 16 * sub + off_ref[sub]
                natural = [ext[pl.ds(start, SUB), :] for ext in (ext_a, ext_b)]
                turned = [pltpu.roll(x, 64, 1) for x in natural]
                rhs_re[sub, pl.ds(row, SUB), :] = jnp.concatenate(natural, axis=1).astype(BF16)
                rhs_im[sub, pl.ds(row, SUB), :] = jnp.concatenate([jnp.where(low, -x, x) for x in turned], axis=1).astype(
                    BF16
                )
                by_four = [
                    jnp.concatenate([ext[pl.ds(start + a, 8, stride=4), :] for a in range(4)], axis=0)
                    for ext in (ext_a, ext_b)
                ]
                lhs_cov[sub, pl.ds(row + 2 * SUB, SUB), :] = jnp.concatenate(by_four, axis=1).astype(BF16)
        return carry

    def tile(g, carry):
        row = pl.multiple_of(g * 128, 128)
        for sub in range(2):
            right = jnp.concatenate([rhs_re[sub, pl.ds(row, 128), :], rhs_im[sub, pl.ds(row, 128), :]], axis=0)
            tiles[sub, pl.ds(pl.multiple_of(g * 256, 256), 256), :] = dot_nt(lhs_cov[sub, pl.ds(row, 256), :], right)
        return carry

    col = lax.broadcasted_iota(jnp.int32, (8, 128), 1)

    def lay_out(g, carry):
        here = pl.multiple_of(g * 256, 256)
        for r in range(4):
            for sub in range(2):
                base = ((g * 4 + r) * 2 + sub) * ROWS
                for part in range(2):
                    lanes = slice(part * 128, part * 128 + 128)
                    by = [[], [], [], []]
                    for b in range(3):
                        block = tiles[sub, pl.ds(here + (r + b + 2) * 32, 32), lanes]
                        if r >= 2:
                            after = tiles[sub, pl.ds(here + 256 + (r + b - 2) * 32, 32), lanes]
                        for a in range(4):
                            x = block[a * 8 : a * 8 + 8]
                            if r >= 2:
                                x = jnp.where(col >= r * 32, x, after[a * 8 : a * 8 + 8])
                            shift = (3 * a - r) % 4 * 32
                            by[a].append((pltpu.roll(x, shift, 1) if shift else x) * (1.0 / 128.0))
                    for u, edge in enumerate((96, 64, 32)):
                        row = jnp.concatenate([jnp.where(col < edge, by[u][b], by[u + 1][b]) for b in range(3)], axis=0)
                        cov[pl.ds(base + 2 * u + part, 24, stride=6), :] = row
        return carry

    done_tiles = done_bins = 0
    for piece, (first, count) in enumerate(PIECES):
        train_copy(piece).wait()

        @pl.when(core == 1)
        def _(piece=piece):
            relay_copy(piece).start()

        same_copy(piece).wait()

        @pl.when(core == 1)
        def _(piece=piece):
            relay_copy(piece).wait()

        @pl.when(core == 0)
        def _(piece=piece):
            cross_copy(piece).wait()

        lax.fori_loop(first // 2, (first + count) // 2, arrange, 0)
        last = piece == len(PIECES) - 1
        ready = HALF // 4 + 1 if last else (first + count - 2) // 4
        lax.fori_loop(done_tiles, ready, tile, 0)
        lax.fori_loop(done_bins, ready - 1, lay_out, 0)
        done_tiles, done_bins = ready, ready - 1
        if piece == 1:
            lax.fori_loop(1, n_b, finish_b, 0)
            sum_a[my_a] = jnp.sum(sum_b[...], axis=0)
            lax.fori_loop(1, n_a, start_a, 0)

    quad_copy.wait()
    quad_sum = send_quad[...] + got_quad[...]
    for sub in range(2):
        quad = quad_sum[:, sub * 64 : sub * 64 + 1] * (1.0 / 128.0) + norms[sub]
        matched_ref[sub] = powers[sub] / quad

    lax.fori_loop(1, n_a, finish_a, 0)
    total = jnp.sum(jnp.sum(sum_a[...], axis=0), axis=1, keepdims=True)
    mean = total * (1.0 / (n_chan * n_rng * 2 * PULSES * GATES)) + 1e-6
    for sub in range(2):
        pmap_ref[sub] = powers[sub] / mean


def hand_out(cov, matched, pmap, cov_out, matched_out, pmap_out, sem):
    pairs = ((cov, cov_out), (matched, matched_out), (pmap, pmap_out))
    copies = [pltpu.make_async_copy(src, dst, sem.at[i]) for i, (src, dst) in enumerate(pairs)]
    for copy in copies:
        copy.start()
    for copy in copies:
        copy.wait()


def local(sizes, radar_cube, offsets, train_index, guard_mask, weights):
    n_z, n_xy, n_chan, n_rng = sizes
    n_a, n_b = n_xy * n_rng, n_z * 2
    n_pieces = len(PIECES)
    dma = pltpu.SemaphoreType.DMA
    vmem = pl.BlockSpec(memory_space=pltpu.VMEM)
    hbm = pl.BlockSpec(memory_space=pltpu.HBM)
    rows = HALF * 2 * ROWS
    shapes = (
        jax.ShapeDtypeStruct((rows, 128), F32),
        jax.ShapeDtypeStruct((2, PULSES, GATES), F32),
        jax.ShapeDtypeStruct((2, PULSES, GATES), F32),
    )
    held = pl.pallas_call(
        functools.partial(kernel, sizes),
        out_shape=shapes,
        in_specs=[hbm] * 6,
        out_specs=(vmem, vmem, vmem),
        scratch_shapes=[
            pltpu.SMEM((2,), jnp.int32),
            pltpu.VMEM((2, CH, PULSES, GATES), BF16),
            pltpu.VMEM((1, TRAIN), jnp.int32),
            pltpu.VMEM((1, GATES), jnp.int32),
            pltpu.VMEM((2, 2, PULSES, 96), BF16),
            pltpu.VMEM((128, 128), BF16),
            pltpu.VMEM((2 * CH * PITCH, GATES), F32),
            pltpu.VMEM((PULSES, 2 * CH, GATES), BF16),
            pltpu.VMEM((PULSES, 2 * CH, GATES), BF16),
            pltpu.VMEM((SLOTS, CH, 128), BF16),
            pltpu.VMEM((SLOTS * HALO, 128), BF16),
            pltpu.VMEM((BINS, CH, 128), BF16),
            pltpu.VMEM((BINS * HALO, 128), BF16),
            pltpu.VMEM((BINS, CH, 128), BF16),
            pltpu.VMEM((3, PULSES, 128), BF16),
            pltpu.VMEM((3, PULSES, 128), BF16),
            pltpu.VMEM((PULSES * 8, 128), F32),
            pltpu.VMEM((PULSES * 8, 128), F32),
            pltpu.VMEM((PULSES * 8, 128), F32),
            pltpu.VMEM((4, PULSES, GATES), F32),
            pltpu.VMEM((4, PULSES, GATES), F32),
            pltpu.VMEM((PULSES, 128), F32),
            pltpu.VMEM((PULSES, 128), F32),
            pltpu.VMEM((n_a, 1, 128), F32),
            pltpu.VMEM((n_b, 1, 128), F32),
            pltpu.VMEM((BINS * EXT, 128), F32),
            pltpu.VMEM((BINS * EXT, 128), F32),
            pltpu.VMEM((2, (BINS + 2) * SUB, 256), BF16),
            pltpu.VMEM((2, (BINS + 2) * SUB, 256), BF16),
            pltpu.VMEM((2, (BINS + 6) * SUB, 256), BF16),
            pltpu.VMEM((2, (HALF // 4 + 1) * 256, 256), F32),
            dma((6,)),
            dma((3,)),
            dma((3,)),
            dma((n_pieces,)),
            dma((n_pieces,)),
            dma((n_pieces,)),
            dma((n_pieces,)),
            dma((n_pieces,)),
            dma((n_pieces,)),
            dma((n_a,)),
            dma((n_a,)),
            dma((n_b,)),
            dma((n_b,)),
        ],
        compiler_params=pltpu.CompilerParams(
            collective_id=0, has_side_effects=True, vmem_limit_bytes=32 * 1024 * 1024
        ),
    )(
        *(
            pltpu.with_memory_space_constraint(x, pltpu.HBM)
            for x in (
                offsets,
                radar_cube,
                train_index.reshape(1, -1),
                guard_mask.reshape(1, -1),
                weights,
                jnp.asarray(dft_matrix()),
            )
        )
    )
    cov, matched, pmap = pl.pallas_call(
        hand_out,
        out_shape=shapes,
        in_specs=[vmem] * 3,
        out_specs=(hbm, hbm, hbm),
        scratch_shapes=[dma((3,))],
        compiler_params=pltpu.CompilerParams(vmem_limit_bytes=1024 * 1024),
    )(*held)
    cov = cov.reshape(HALF, 2, ROWS // 2, 2, 128).transpose(0, 1, 3, 2, 4).reshape(HALF, 2, 2, ROWS * 64)
    return cov, matched, pmap


def solution(mesh):
    n_chan, n_rng = mesh.shape["chan"], mesh.shape["rng"]
    n_xy = 8 if n_chan >= 64 else 2
    sizes = (n_chan // (2 * n_xy), n_xy, n_chan, n_rng)
    return jax.shard_map(
        functools.partial(local, sizes),
        mesh=mesh,
        in_specs=(
            P(None, "chan", None, "rng"),
            P("chan"),
            P("rng"),
            P("rng"),
            P(None, "chan", None, None),
        ),
        out_specs=(P("rng", "chan", None, None), P("chan", None, "rng"), P("chan", None, "rng")),
        check_vma=False,
    )
```

```python
import functools
import math

import jax
import jax.numpy as jnp
import numpy as np
from jax import lax
from jax.experimental import pallas as pl
from jax.experimental.pallas import tpu as pltpu
from jax.sharding import PartitionSpec as P

MESH = pl.DeviceIdType.MESH
F32 = jnp.float32
BF16 = jnp.bfloat16

PULSES = 64
CH = 32
SUB = 32
HALO = 24
EXT = CH + HALO
GATES = 128
TRAIN = 64
HALF = 32
BINS = HALF + 2
SLOTS = PULSES + 2
GROUP = 22
ROWS = 144
PARTS = 4
PITCH = PULSES + 8
PIECES = ((0, 10), (10, 8), (18, 8), (26, 8))


def dft_matrix():
    freq = np.arange(PULSES)
    angle = (freq[:, None] * freq[None, :] % PULSES) * (2.0 * math.pi / PULSES)
    cosine = np.cos(angle) / math.sqrt(PULSES)
    sine = np.sin(angle) / math.sqrt(PULSES)
    return np.block([[cosine, sine], [-sine, cosine]]).astype(jnp.bfloat16)


def dot(a, b):
    return jnp.dot(a, b, preferred_element_type=F32)


def dot_nt(a, b):
    return lax.dot_general(a, b, (((1,), (1,)), ((), ())), preferred_element_type=F32)


def turned_by(x, shift):
    return pltpu.roll(x, shift % x.shape[0], 0) if shift else x


def kernel(
    sizes,
    off_hbm,
    cube_hbm,
    idx_hbm,
    guard_hbm,
    wts_hbm,
    dft_hbm,
    cov,
    matched_ref,
    pmap_ref,
    off_ref,
    cube,
    idx_ref,
    guard_ref,
    wts_ref,
    dft_ref,
    spec,
    bins,
    train,
    train_halo,
    got_train,
    got_same,
    got_cross,
    send_wts,
    got_wts,
    lhs_re,
    lhs_im,
    filt_re,
    filt_im,
    send_part,
    got_part,
    send_quad,
    got_quad,
    sum_a,
    sum_b,
    ext_a,
    ext_b,
    rhs_re,
    rhs_im,
    lhs_cov,
    tiles,
    fetch_sem,
    send_sem,
    recv_sem,
    train_recv,
    same_recv,
    cross_recv,
):
    n_z, n_xy, n_chan, n_rng = sizes
    n_a, n_b = n_xy * n_rng, n_z * 2
    chan, rng = lax.axis_index("chan"), lax.axis_index("rng")
    other = 1 - rng
    prev, following = lax.rem(chan + n_chan - 1, n_chan), lax.rem(chan + 1, n_chan)
    core = lax.rem(chan, 2)
    chip = chan // 2
    z, xy = chip // n_xy, lax.rem(chip, n_xy)
    my_a, my_b = xy * n_rng + rng, z * 2 + core

    def peer_a(step):
        slot = lax.rem(my_a + step, n_a)
        return (z * n_xy + slot // n_rng) * 2 + core, lax.rem(slot, n_rng)

    def peer_b(step):
        slot = lax.rem(my_b + step, n_b)
        return ((slot // 2) * n_xy + xy) * 2 + lax.rem(slot, 2), rng

    def remote(src, dst, send, recv, device):
        return pltpu.make_async_remote_copy(
            src_ref=src,
            dst_ref=dst,
            send_sem=send,
            recv_sem=recv,
            device_id=device,
            device_id_type=MESH,
        )

    fetches = [
        pltpu.make_async_copy(src, dst, fetch_sem.at[i])
        for i, (src, dst) in enumerate(
            (
                (off_hbm, off_ref),
                (wts_hbm, wts_ref),
                (idx_hbm, idx_ref),
                (guard_hbm, guard_ref),
                (dft_hbm, dft_ref),
                (cube_hbm, cube),
            )
        )
    ]
    for fetch in fetches:
        fetch.start()
    barrier = pltpu.get_barrier_semaphore()
    for device in ((prev, rng), (following, rng), (prev, other), (following, other)):
        pl.semaphore_signal(barrier, inc=1, device_id=device, device_id_type=MESH)

    for step in range(1, n_b):
        pl.semaphore_signal(barrier, inc=1, device_id=peer_b(step), device_id_type=MESH)
    for step in range(1, n_a):
        pl.semaphore_signal(barrier, inc=1, device_id=peer_a(step), device_id_type=MESH)

    fetches[0].wait()
    fetches[1].wait()
    lane = lax.broadcasted_iota(jnp.int32, (1, 128), 1)
    depth = lax.broadcasted_iota(jnp.int32, (96, 128), 0)
    placed = [[jnp.zeros((PULSES, 128), F32) for _ in range(3)] for _ in range(2)]
    for sub in range(2):
        for part in range(2):
            value = wts_ref[part, sub]
            for ahead in range(2):
                at = lax.rem(lane, 32) + (32 * ahead - 16 * sub) - off_ref[sub]
                fits = (at >= 0) & (at < SUB) & (lane // 32 == sub * 2 + part)
                for b in range(3):
                    hot = jnp.where(depth == jnp.where(fits, at + b * SUB, -1), 1.0, 0.0).astype(BF16)
                    placed[ahead][b] = placed[ahead][b] + dot(value, hot)
    for b in range(3):
        send_wts[b] = turned_by(placed[1][b], b - 1).astype(BF16)

    first_half = lax.rem(lax.broadcasted_iota(jnp.int32, (PULSES, 128), 1), 64) < 32

    def fill_lhs(tables):
        for b in range(3):
            x = tables[b]
            up, down = pltpu.roll(x, 96, 1), pltpu.roll(x, 32, 1)
            lhs_re[pl.ds(b * 2, PULSES, stride=8), :] = x
            lhs_re[pl.ds(b * 2 + 1, PULSES, stride=8), :] = pltpu.roll(x, 64, 1)
            lhs_im[pl.ds(b * 2, PULSES, stride=8), :] = jnp.where(first_half, -up, down)
            lhs_im[pl.ds(b * 2 + 1, PULSES, stride=8), :] = jnp.where(first_half, -down, up)

    fetches[2].wait()
    fetches[3].wait()
    gate = lax.broadcasted_iota(jnp.int32, (GATES, 128), 0)
    wanted = jnp.concatenate([idx_ref[...], idx_ref[...]], axis=1)
    hits = jnp.where(gate == wanted, 1.0, 0.0)
    guard = jnp.broadcast_to(guard_ref[...].astype(F32), (8, GATES)).astype(BF16)
    keep = dot(guard, hits.astype(BF16))[0:1]
    pick = (hits * keep).astype(BF16)
    counts = dot_nt(jnp.full((8, 128), 0.5, BF16), pick)[0:1]

    fetches[4].wait()
    fetches[5].wait()
    table = dft_ref[...]

    def doppler(step, carry):
        for u in range(4):
            m = step * 8 + 2 * u
            pair = [jnp.concatenate([cube[0, m + v], cube[1, m + v]], axis=0) for v in range(2)]
            out = dot(table, jnp.concatenate(pair, axis=1))
            for v in range(2):
                for part in range(2):
                    start = pl.multiple_of((part * CH + m + v) * PITCH, 8)
                    spec[pl.ds(start, PULSES), :] = out[part * 64 : part * 64 + 64, v * 128 : v * 128 + 128]
        return carry

    lax.fori_loop(0, CH // 8, doppler, 0)

    pl.semaphore_wait(barrier, 4 + (n_a - 1) + (n_b - 1))
    wts_copy = remote(send_wts, got_wts, send_sem.at[0], recv_sem.at[0], (following, rng))
    wts_copy.start()

    left = lax.broadcasted_iota(jnp.int32, (CH, 128), 1) < TRAIN

    def gather_bins(step):
        for u in range(GROUP):
            k = lax.rem(step * GROUP + u + PULSES - 1, PULSES)
            re = spec[pl.ds(k, CH, stride=PITCH), :]
            im = spec[pl.ds(k + CH * PITCH, CH, stride=PITCH), :]
            bins[k] = jnp.concatenate([re, im], axis=0).astype(BF16)

    def choose_gates(step):
        rows = [bins[lax.rem(step * GROUP + u + PULSES - 1, PULSES)] for u in range(GROUP)]
        chosen = dot(jnp.concatenate(rows, axis=0), pick)
        halo = []
        for u in range(GROUP):
            tile = jnp.where(left, chosen[u * 64 : u * 64 + 32], chosen[u * 64 + 32 : u * 64 + 64])
            train[step * GROUP + u] = tile.astype(BF16)
            halo.append(tile[:HALO])
        start = pl.multiple_of(step * (GROUP * HALO), GROUP * HALO)
        train_halo[pl.ds(start, GROUP * HALO), :] = jnp.concatenate(halo, axis=0).astype(BF16)

    def per_bin(step, carry):
        choose_gates(step - 1)
        gather_bins(step)
        return carry

    gather_bins(0)
    lax.fori_loop(1, SLOTS // GROUP, per_bin, 0)
    choose_gates(SLOTS // GROUP - 1)

    def train_copy(piece):
        first, count = PIECES[piece]
        return remote(
            train.at[pl.ds(other * HALF + first, count)],
            got_train.at[pl.ds(first, count)],
            send_sem.at[3],
            train_recv.at[piece],
            (chan, other),
        )

    def same_copy(piece):
        first, count = PIECES[piece]
        start = pl.multiple_of(rng * (HALF * HALO) + first * HALO, 16)
        return remote(
            train_halo.at[pl.ds(start, count * HALO)],
            got_same.at[pl.ds(first * HALO, count * HALO)],
            send_sem.at[4],
            same_recv.at[piece],
            (prev, rng),
        )

    def cross_copy(piece):
        first, count = PIECES[piece]
        return remote(
            train.at[pl.ds(other * HALF + first, count)],
            got_cross.at[pl.ds(first, count)],
            send_sem.at[5],
            cross_recv.at[piece],
            (prev, other),
        )

    def relay_copy(piece):
        first, count = PIECES[piece]
        return remote(
            got_train.at[pl.ds(first, count)],
            got_cross.at[pl.ds(first, count)],
            send_sem.at[5],
            cross_recv.at[piece],
            (prev, rng),
        )

    def send_piece(piece):
        train_copy(piece).start()

        @pl.when(core == 0)
        def _():
            same_copy(piece).start()
            cross_copy(piece).start()

    send_piece(0)

    @pl.when(core == 1)
    def _():
        for piece in range(len(PIECES)):
            same_copy(piece).start()

    def filtered():
        def one(step, carry):
            for u in range(32):
                k = step * 32 + u
                row = pl.multiple_of(k * 8, 8)
                weight = jnp.concatenate([lhs_re[pl.ds(row, 8), :], lhs_im[pl.ds(row, 8), :]], axis=0)
                out = dot(weight[:, :64].astype(BF16), bins[k])
                filt_re[pl.ds(row, 8), :] = out[:8]
                filt_im[pl.ds(row, 8), :] = out[8:]
            return carry

        lax.fori_loop(0, PULSES // 32, one, 0)
        sums = []
        for sub in range(2):
            for ref in (filt_re, filt_im):
                terms = [turned_by(ref[pl.ds(b * 2 + sub, PULSES, stride=8), :], 1 - b) for b in range(3)]
                sums.append(terms[0] + terms[1] + terms[2])
        return sums

    wts_copy.wait()
    fill_lhs([got_wts[b].astype(F32) for b in range(3)])
    for part, value in enumerate(filtered()):
        send_part[part] = value
    part_copy = remote(send_part, got_part, send_sem.at[1], recv_sem.at[1], (prev, rng))
    part_copy.start()

    fill_lhs([turned_by(placed[0][b], b - 1) for b in range(3)])
    own = filtered()

    norms = []
    for sub in range(2):
        re, im = wts_ref[0, sub].astype(F32), wts_ref[1, sub].astype(F32)
        norms.append(jnp.sum(re * re + im * im, axis=1, keepdims=True))

    def spread(ref, peers, sem, peer):
        for step in range(1, peers):
            remote(ref.at[peers - 1], ref.at[step - 1], send_sem.at[sem], recv_sem.at[sem - 3], peer(step)).start()

    def collect(ref, peers, sem, peer):
        span = ref.at[pl.ds(0, peers - 1)]
        remote(span, span, send_sem.at[sem], recv_sem.at[sem - 3], peer(1)).wait()

    low = lax.broadcasted_iota(jnp.int32, (SUB, 128), 1) < TRAIN

    def arrange(step, carry):
        rows = pl.multiple_of(step * (2 * HALO), 2 * HALO)
        same = got_same[pl.ds(rows, 2 * HALO), :].astype(F32)
        for u in range(2):
            k = step * 2 + u
            start = pl.multiple_of(k * EXT, 8)
            ext_a[pl.ds(start, CH), :] = train[rng * HALF + k].astype(F32)
            ext_a[pl.ds(start + CH, HALO), :] = same[u * HALO : u * HALO + HALO]
            ext_b[pl.ds(start, CH), :] = got_train[k].astype(F32)
            ext_b[pl.ds(start + CH, HALO), :] = got_cross[k].astype(F32)[:HALO]
        for u in range(2):
            k = step * 2 + u
            row = pl.multiple_of(k * SUB, SUB)
            for sub in range(2):
                start = k * EXT + 16 * sub + off_ref[sub]
                natural = [ext[pl.ds(start, SUB), :] for ext in (ext_a, ext_b)]
                turned = [pltpu.roll(x, 64, 1) for x in natural]
                rhs_re[sub, pl.ds(row, SUB), :] = jnp.concatenate(natural, axis=1).astype(BF16)
                rhs_im[sub, pl.ds(row, SUB), :] = jnp.concatenate([jnp.where(low, -x, x) for x in turned], axis=1).astype(
                    BF16
                )
                by_four = [
                    jnp.concatenate([ext[pl.ds(start + a, 8, stride=4), :] for a in range(4)], axis=0)
                    for ext in (ext_a, ext_b)
                ]
                lhs_cov[sub, pl.ds(row + 2 * SUB, SUB), :] = jnp.concatenate(by_four, axis=1).astype(BF16)
        return carry

    def tile(g):
        row = g * 128
        for sub in range(2):
            right = jnp.concatenate([rhs_re[sub, pl.ds(row, 128), :], rhs_im[sub, pl.ds(row, 128), :]], axis=0)
            tiles[sub, pl.ds(g * 256, 256), :] = dot_nt(lhs_cov[sub, pl.ds(row, 256), :], right)

    col = lax.broadcasted_iota(jnp.int32, (8, 128), 1)

    def lay_out(g, carry):
        here = pl.multiple_of(g * 256, 256)
        for r in range(4):
            for sub in range(2):
                base = ((g * 4 + r) * 2 + sub) * ROWS
                for part in range(2):
                    lanes = slice(part * 128, part * 128 + 128)
                    by = [[], [], [], []]
                    for b in range(3):
                        block = tiles[sub, pl.ds(here + (r + b + 2) * 32, 32), lanes]
                        if r >= 2:
                            after = tiles[sub, pl.ds(here + 256 + (r + b - 2) * 32, 32), lanes]
                        for a in range(4):
                            x = block[a * 8 : a * 8 + 8]
                            if r >= 2:
                                x = jnp.where(col >= r * 32, x, after[a * 8 : a * 8 + 8])
                            shift = (3 * a - r) % 4 * 32
                            by[a].append((pltpu.roll(x, shift, 1) if shift else x) * (1.0 / 128.0))
                    for u, edge in enumerate((96, 64, 32)):
                        row = jnp.concatenate([jnp.where(col < edge, by[u][b], by[u + 1][b]) for b in range(3)], axis=0)
                        cov[pl.ds(base + 2 * u + part, 24, stride=6), :] = row
        return carry

    def pass_on(piece):
        train_copy(piece).wait_recv()

        @pl.when(core == 1)
        def _():
            relay_copy(piece).start()

    ready = [(first + count - 2) // 4 for first, count in PIECES]
    ready[-1] = HALF // 4 + 1

    def cover(piece):
        first, count = PIECES[piece]
        same_copy(piece).wait_recv()
        relay_copy(piece).wait_recv()
        lax.fori_loop(first // 2, (first + count) // 2, arrange, 0)
        begin = ready[piece - 1] if piece else 0
        for g in range(begin, ready[piece]):
            tile(g)
        lax.fori_loop(max(begin - 1, 0), ready[piece] - 1, lay_out, 0)

    pass_on(0)
    cover(0)
    part_copy.wait()
    powers = []
    for sub in range(2):
        re = own[2 * sub] + got_part[2 * sub]
        im = own[2 * sub + 1] + got_part[2 * sub + 1]
        powers.append(re * re + im * im)
    sum_a[n_a - 1] = jnp.sum(powers[0] + powers[1], axis=0, keepdims=True)

    spread(sum_a, n_a, 7, peer_a)
    for piece in range(1, len(PIECES)):
        send_piece(piece)
    quads = [jnp.sum(p * counts, axis=1, keepdims=True) for p in powers]
    send_quad[...] = jnp.where(lane < 64, quads[0], quads[1])
    quad_copy = remote(send_quad, got_quad, send_sem.at[2], recv_sem.at[2], (chan, other))
    quad_copy.start()


    pass_on(1)
    cover(1)

    collect(sum_a, n_a, 7, peer_a)
    sum_b[n_b - 1] = jnp.sum(sum_a[...], axis=0)
    spread(sum_b, n_b, 6, peer_b)
    pass_on(2)
    cover(2)
    pass_on(3)
    cover(3)

    quad_copy.wait()
    quad_sum = send_quad[...] + got_quad[...]
    for sub in range(2):
        quad = quad_sum[:, sub * 64 : sub * 64 + 1] * (1.0 / 128.0) + norms[sub]
        matched_ref[sub] = powers[sub] / quad

    collect(sum_b, n_b, 6, peer_b)
    total = jnp.sum(jnp.sum(sum_b[...], axis=0), axis=1, keepdims=True)
    mean = total * (1.0 / (n_chan * n_rng * 2 * PULSES * GATES)) + 1e-6
    for sub in range(2):
        pmap_ref[sub] = powers[sub] / mean
    train_span, halo_span = train.at[pl.ds(0, BINS)], train_halo.at[pl.ds(0, BINS * HALO)]
    remote(train_span, got_train, send_sem.at[3], train_recv.at[0], (chan, other)).wait_send()
    remote(halo_span, got_same, send_sem.at[4], same_recv.at[0], (prev, rng)).wait_send()
    remote(train_span, got_cross, send_sem.at[5], cross_recv.at[0], (prev, rng)).wait_send()


def hand_out(cov, matched, pmap, cov_out, matched_out, pmap_out, sem):
    rows = cov.shape[0] // PARTS
    parts = [(cov.at[pl.ds(i * rows, rows)], cov_out.at[pl.ds(i * rows, rows)]) for i in range(PARTS)]
    pairs = (*parts, (matched, matched_out), (pmap, pmap_out))
    copies = [pltpu.make_async_copy(src, dst, sem.at[i]) for i, (src, dst) in enumerate(pairs)]
    for copy in copies:
        copy.start()
    for copy in copies:
        copy.wait()


def local(sizes, radar_cube, offsets, train_index, guard_mask, weights):
    n_z, n_xy, n_chan, n_rng = sizes
    n_a, n_b = n_xy * n_rng, n_z * 2
    n_pieces = len(PIECES)
    dma = pltpu.SemaphoreType.DMA
    vmem = pl.BlockSpec(memory_space=pltpu.VMEM)
    hbm = pl.BlockSpec(memory_space=pltpu.HBM)
    rows = HALF * 2 * ROWS
    shapes = (
        jax.ShapeDtypeStruct((rows, 128), F32),
        jax.ShapeDtypeStruct((2, PULSES, GATES), F32),
        jax.ShapeDtypeStruct((2, PULSES, GATES), F32),
    )
    held = pl.pallas_call(
        functools.partial(kernel, sizes),
        out_shape=shapes,
        in_specs=[hbm] * 6,
        out_specs=(vmem, vmem, vmem),
        scratch_shapes=[
            pltpu.SMEM((2,), jnp.int32),
            pltpu.VMEM((2, CH, PULSES, GATES), BF16),
            pltpu.VMEM((1, TRAIN), jnp.int32),
            pltpu.VMEM((1, GATES), jnp.int32),
            pltpu.VMEM((2, 2, PULSES, 96), BF16),
            pltpu.VMEM((128, 128), BF16),
            pltpu.VMEM((2 * CH * PITCH, GATES), F32),
            pltpu.VMEM((PULSES, 2 * CH, GATES), BF16),
            pltpu.VMEM((SLOTS, CH, 128), BF16),
            pltpu.VMEM((SLOTS * HALO, 128), BF16),
            pltpu.VMEM((BINS, CH, 128), BF16),
            pltpu.VMEM((BINS * HALO, 128), BF16),
            pltpu.VMEM((BINS, CH, 128), BF16),
            pltpu.VMEM((3, PULSES, 128), BF16),
            pltpu.VMEM((3, PULSES, 128), BF16),
            pltpu.VMEM((PULSES * 8, 128), F32),
            pltpu.VMEM((PULSES * 8, 128), F32),
            pltpu.VMEM((PULSES * 8, 128), F32),
            pltpu.VMEM((PULSES * 8, 128), F32),
            pltpu.VMEM((4, PULSES, GATES), F32),
            pltpu.VMEM((4, PULSES, GATES), F32),
            pltpu.VMEM((PULSES, 128), F32),
            pltpu.VMEM((PULSES, 128), F32),
            pltpu.VMEM((n_a, 1, 128), F32),
            pltpu.VMEM((n_b, 1, 128), F32),
            pltpu.VMEM((BINS * EXT, 128), F32),
            pltpu.VMEM((BINS * EXT, 128), F32),
            pltpu.VMEM((2, (BINS + 2) * SUB, 256), BF16),
            pltpu.VMEM((2, (BINS + 2) * SUB, 256), BF16),
            pltpu.VMEM((2, (BINS + 6) * SUB, 256), BF16),
            pltpu.VMEM((2, (HALF // 4 + 1) * 256, 256), F32),
            dma((6,)),
            dma((8,)),
            dma((5,)),
            dma((n_pieces,)),
            dma((n_pieces,)),
            dma((n_pieces,)),
        ],
        compiler_params=pltpu.CompilerParams(
            collective_id=0, has_side_effects=True, vmem_limit_bytes=32 * 1024 * 1024
        ),
    )(
        *(
            pltpu.with_memory_space_constraint(x, pltpu.HBM)
            for x in (
                offsets,
                radar_cube,
                train_index.reshape(1, -1),
                guard_mask.reshape(1, -1),
                weights,
                jnp.asarray(dft_matrix()),
            )
        )
    )
    cov, matched, pmap = pl.pallas_call(
        hand_out,
        out_shape=shapes,
        in_specs=[vmem] * 3,
        out_specs=(hbm, hbm, hbm),
        scratch_shapes=[dma((PARTS + 2,))],
        compiler_params=pltpu.CompilerParams(vmem_limit_bytes=1024 * 1024),
    )(*held)
    cov = cov.reshape(HALF, 2, ROWS // 2, 2, 128).transpose(0, 1, 3, 2, 4).reshape(HALF, 2, 2, ROWS * 64)
    return cov, matched, pmap


def solution(mesh):
    n_chan, n_rng = mesh.shape["chan"], mesh.shape["rng"]
    n_xy = 8 if n_chan >= 64 else 2
    sizes = (n_chan // (2 * n_xy), n_xy, n_chan, n_rng)
    return jax.shard_map(
        functools.partial(local, sizes),
        mesh=mesh,
        in_specs=(
            P(None, "chan", None, "rng"),
            P("chan"),
            P("rng"),
            P("rng"),
            P(None, "chan", None, None),
        ),
        out_specs=(P("rng", "chan", None, None), P("chan", None, "rng"), P("chan", None, "rng")),
        check_vma=False,
    )
```

```python
import functools
import math

import jax
import jax.numpy as jnp
import numpy as np
from jax import lax
from jax.experimental import pallas as pl
from jax.experimental.pallas import tpu as pltpu
from jax.sharding import PartitionSpec as P

MESH = pl.DeviceIdType.MESH
F32 = jnp.float32
BF16 = jnp.bfloat16

PULSES = 64
CH = 32
SUB = 32
HALO = 24
EXT = CH + HALO
GATES = 128
TRAIN = 64
HALF = 32
BINS = HALF + 2
SLOTS = PULSES + 2
GROUP = 22
HEAD = 3
ROWS = 144
PITCH = PULSES + 8
PIECES = ((0, 10), (10, 8), (18, 8), (26, 8))


def dft_matrix():
    freq = np.arange(PULSES)
    angle = (freq[:, None] * freq[None, :] % PULSES) * (2.0 * math.pi / PULSES)
    cosine = np.cos(angle) / math.sqrt(PULSES)
    sine = np.sin(angle) / math.sqrt(PULSES)
    return np.block([[cosine, sine], [-sine, cosine]]).astype(jnp.bfloat16)


def dot(a, b):
    return jnp.dot(a, b, preferred_element_type=F32)


def dot_nt(a, b):
    return lax.dot_general(a, b, (((1,), (1,)), ((), ())), preferred_element_type=F32)


def turned_by(x, shift):
    return pltpu.roll(x, shift % x.shape[0], 0) if shift else x


def lay_out(tiles, cov, origin, g, carry):
    col = lax.broadcasted_iota(jnp.int32, (8, 128), 1)
    here = pl.multiple_of(g * 256, 256)
    for r in range(4):
        for sub in range(2):
            base = (((g - origin) * 4 + r) * 2 + sub) * ROWS
            for part in range(2):
                lanes = slice(part * 128, part * 128 + 128)
                by = [[], [], [], []]
                for b in range(3):
                    block = tiles[sub, pl.ds(here + (r + b + 2) * 32, 32), lanes]
                    if r >= 2:
                        after = tiles[sub, pl.ds(here + 256 + (r + b - 2) * 32, 32), lanes]
                    for a in range(4):
                        x = block[a * 8 : a * 8 + 8]
                        if r >= 2:
                            x = jnp.where(col >= r * 32, x, after[a * 8 : a * 8 + 8])
                        shift = (3 * a - r) % 4 * 32
                        by[a].append(pltpu.roll(x, shift, 1) if shift else x)
                for u, edge in enumerate((96, 64, 32)):
                    row = jnp.concatenate([jnp.where(col < edge, by[u][b], by[u + 1][b]) for b in range(3)], axis=0)
                    cov[pl.ds(base + 2 * u + part, 24, stride=6), :] = row
    return carry


def kernel(
    sizes,
    off_hbm,
    cube_hbm,
    idx_hbm,
    guard_hbm,
    wts_hbm,
    dft_hbm,
    tiles,
    head,
    matched_ref,
    pmap_ref,
    off_ref,
    cube,
    idx_ref,
    guard_ref,
    wts_ref,
    dft_ref,
    spec,
    bins,
    train,
    train_halo,
    got_train,
    got_same,
    got_cross,
    send_wts,
    got_wts,
    lhs_re,
    lhs_im,
    filt_re,
    filt_im,
    send_part,
    got_part,
    send_quad,
    got_quad,
    sum_a,
    sum_b,
    ext_a,
    ext_b,
    rhs_re,
    rhs_im,
    lhs_cov,
    fetch_sem,
    send_sem,
    recv_sem,
    train_recv,
    same_recv,
    cross_recv,
):
    n_z, n_xy, n_chan, n_rng = sizes
    n_a, n_b = n_xy * n_rng, n_z * 2
    chan, rng = lax.axis_index("chan"), lax.axis_index("rng")
    other = 1 - rng
    prev, following = lax.rem(chan + n_chan - 1, n_chan), lax.rem(chan + 1, n_chan)
    core = lax.rem(chan, 2)
    chip = chan // 2
    z, xy = chip // n_xy, lax.rem(chip, n_xy)
    my_a, my_b = xy * n_rng + rng, z * 2 + core

    def peer_a(step):
        slot = lax.rem(my_a + step, n_a)
        return (z * n_xy + slot // n_rng) * 2 + core, lax.rem(slot, n_rng)

    def peer_b(step):
        slot = lax.rem(my_b + step, n_b)
        return ((slot // 2) * n_xy + xy) * 2 + lax.rem(slot, 2), rng

    def remote(src, dst, send, recv, device):
        return pltpu.make_async_remote_copy(
            src_ref=src,
            dst_ref=dst,
            send_sem=send,
            recv_sem=recv,
            device_id=device,
            device_id_type=MESH,
        )

    fetches = [
        pltpu.make_async_copy(src, dst, fetch_sem.at[i])
        for i, (src, dst) in enumerate(
            (
                (off_hbm, off_ref),
                (wts_hbm, wts_ref),
                (idx_hbm, idx_ref),
                (guard_hbm, guard_ref),
                (dft_hbm, dft_ref),
                (cube_hbm, cube),
            )
        )
    ]
    for i in (1, 0, 5, 4):
        fetches[i].start()
    barrier = pltpu.get_barrier_semaphore()
    for device in ((prev, rng), (following, rng), (prev, other), (following, other)):
        pl.semaphore_signal(barrier, inc=1, device_id=device, device_id_type=MESH)

    for step in range(1, n_b):
        pl.semaphore_signal(barrier, inc=1, device_id=peer_b(step), device_id_type=MESH)
    for step in range(1, n_a):
        pl.semaphore_signal(barrier, inc=1, device_id=peer_a(step), device_id_type=MESH)
    for fetch in fetches[2:4]:
        fetch.start()

    fetches[0].wait()
    fetches[1].wait()
    lane = lax.broadcasted_iota(jnp.int32, (1, 128), 1)
    depth = lax.broadcasted_iota(jnp.int32, (96, 128), 0)
    placed = [[jnp.zeros((PULSES, 128), F32) for _ in range(3)] for _ in range(2)]
    group, place = lane // 32, lax.rem(lane, 32)
    for sub in range(2):
        for part in range(2):
            value = wts_ref[part, sub]
            for ahead in range(2):
                if ahead:
                    channel = CH + (place if sub else place - HALO)
                    mine = (group == part) & ((place < HALO) if sub else (place >= HALO))
                else:
                    channel = place
                    mine = group == sub * 2 + part
                at = channel - 16 * sub - off_ref[sub]
                fits = (at >= 0) & (at < SUB) & mine
                for b in range(3):
                    hot = jnp.where(depth == jnp.where(fits, at + b * SUB, -1), 1.0, 0.0).astype(BF16)
                    placed[ahead][b] = placed[ahead][b] + dot(value, hot)
    for b in range(3):
        turned = turned_by(placed[1][b], b - 1)
        send_wts[b] = (turned[:32] + pltpu.roll(turned[32:], 64, 1)).astype(BF16)

    wide = lax.broadcasted_iota(jnp.int32, (PULSES, 128), 1)

    def fill_lhs(b, sub, x):
        lhs_re[pl.ds(b * 2 + sub, PULSES, stride=8), :] = x
        lhs_im[pl.ds(b * 2 + sub, PULSES, stride=8), :] = jnp.where(
            wide < 32, -pltpu.roll(x, 96, 1), pltpu.roll(x, 32, 1)
        )

    fetches[4].wait()
    fetches[5].wait()
    table = dft_ref[...]

    def doppler(step, carry):
        for u in range(4):
            m = step * 8 + 2 * u
            pair = [jnp.concatenate([cube[0, m + v], cube[1, m + v]], axis=0) for v in range(2)]
            out = dot(table, jnp.concatenate(pair, axis=1))
            for v in range(2):
                for part in range(2):
                    start = pl.multiple_of((part * CH + m + v) * PITCH, 8)
                    spec[pl.ds(start, PULSES), :] = out[part * 64 : part * 64 + 64, v * 128 : v * 128 + 128]
        return carry

    lax.fori_loop(0, CH // 8, doppler, 0)

    pl.semaphore_wait(barrier, 4 + (n_a - 1) + (n_b - 1))
    wts_copy = remote(send_wts, got_wts, send_sem.at[0], recv_sem.at[0], (following, rng))
    wts_copy.start()

    fetches[2].wait()
    fetches[3].wait()
    gate = lax.broadcasted_iota(jnp.int32, (GATES, 128), 0)
    wanted = jnp.concatenate([idx_ref[...], idx_ref[...]], axis=1)
    hits = jnp.where(gate == wanted, 1.0, 0.0)
    guard = jnp.broadcast_to(guard_ref[...].astype(F32), (8, GATES)).astype(BF16)
    keep = dot(guard, hits.astype(BF16))[0:1]
    pick = (hits * keep).astype(BF16)
    counts = dot_nt(jnp.full((8, 128), 0.5, BF16), pick)[0:1]

    left = lax.broadcasted_iota(jnp.int32, (CH, 128), 1) < TRAIN

    def gather_bins(step):
        for u in range(GROUP):
            k = lax.rem(step * GROUP + u + PULSES - 1, PULSES)
            re = spec[pl.ds(k, CH, stride=PITCH), :]
            im = spec[pl.ds(k + CH * PITCH, CH, stride=PITCH), :]
            bins[k] = jnp.concatenate([re, im], axis=0).astype(BF16)

    def choose_gates(step):
        rows = [bins[lax.rem(step * GROUP + u + PULSES - 1, PULSES)] for u in range(GROUP)]
        chosen = dot(jnp.concatenate(rows, axis=0), pick)
        halo = []
        for u in range(GROUP):
            tile = jnp.where(left, chosen[u * 64 : u * 64 + 32], chosen[u * 64 + 32 : u * 64 + 64])
            train[step * GROUP + u] = tile.astype(BF16)
            halo.append(tile[:HALO])
        start = pl.multiple_of(step * (GROUP * HALO), GROUP * HALO)
        train_halo[pl.ds(start, GROUP * HALO), :] = jnp.concatenate(halo, axis=0).astype(BF16)

    def per_bin(step, carry):
        choose_gates(step - 1)
        gather_bins(step)
        return carry

    gather_bins(0)
    lax.fori_loop(1, SLOTS // GROUP, per_bin, 0)
    choose_gates(SLOTS // GROUP - 1)

    def train_copy(piece):
        first, count = PIECES[piece]
        return remote(
            train.at[pl.ds(other * HALF + first, count)],
            got_train.at[pl.ds(first, count)],
            send_sem.at[3],
            train_recv.at[piece],
            (chan, other),
        )

    def same_copy(piece):
        first, count = PIECES[piece]
        start = pl.multiple_of(rng * (HALF * HALO) + first * HALO, 16)
        return remote(
            train_halo.at[pl.ds(start, count * HALO)],
            got_same.at[pl.ds(first * HALO, count * HALO)],
            send_sem.at[4],
            same_recv.at[piece],
            (prev, rng),
        )

    def cross_copy(piece):
        first, count = PIECES[piece]
        return remote(
            train.at[pl.ds(other * HALF + first, count)],
            got_cross.at[pl.ds(first, count)],
            send_sem.at[5],
            cross_recv.at[piece],
            (prev, other),
        )

    def relay_copy(piece):
        first, count = PIECES[piece]
        return remote(
            got_train.at[pl.ds(first, count)],
            got_cross.at[pl.ds(first, count)],
            send_sem.at[5],
            cross_recv.at[piece],
            (prev, rng),
        )

    def send_piece(piece):
        train_copy(piece).start()

        @pl.when(core == 0)
        def _():
            same_copy(piece).start()
            cross_copy(piece).start()

    send_piece(0)

    @pl.when(core == 1)
    def _():
        for piece in range(len(PIECES)):
            same_copy(piece).start()

    def filtered():
        def one(step, carry):
            for u in range(32):
                k = step * 32 + u
                row = pl.multiple_of(k * 8, 8)
                weight = jnp.concatenate([lhs_re[pl.ds(row, 8), :], lhs_im[pl.ds(row, 8), :]], axis=0)
                out = dot(weight[:, :64].astype(BF16), bins[k])
                filt_re[pl.ds(row, 8), :] = out[:8]
                filt_im[pl.ds(row, 8), :] = out[8:]
            return carry

        lax.fori_loop(0, PULSES // 32, one, 0)
        sums = []
        for sub in range(2):
            for ref in (filt_re, filt_im):
                terms = [turned_by(ref[pl.ds(b * 2 + sub, PULSES, stride=8), :], 1 - b) for b in range(3)]
                sums.append(terms[0] + terms[1] + terms[2])
        return sums

    wts_copy.wait()
    for b in range(3):
        packed = got_wts[b].astype(F32)
        table = jnp.concatenate([packed, pltpu.roll(packed, 64, 1)], axis=0)
        fill_lhs(b, 1, jnp.where(lax.rem(wide, 32) < HALO, table, 0.0))
        fill_lhs(b, 0, jnp.where(lax.rem(wide, 32) < CH - HALO, pltpu.roll(table, 128 - HALO, 1), 0.0))
    for part, value in enumerate(filtered()):
        send_part[part] = value
    part_copy = remote(send_part, got_part, send_sem.at[1], recv_sem.at[1], (prev, rng))
    part_copy.start()

    for b in range(3):
        turned = turned_by(placed[0][b], b - 1)
        fill_lhs(b, 0, turned)
        fill_lhs(b, 1, pltpu.roll(turned, 64, 1))
    own = filtered()

    norms = []
    for sub in range(2):
        re, im = wts_ref[0, sub].astype(F32), wts_ref[1, sub].astype(F32)
        norms.append(jnp.sum(re * re + im * im, axis=1, keepdims=True))

    def spread(ref, peers, sem, peer):
        for step in range(1, peers):
            remote(ref.at[peers - 1], ref.at[step - 1], send_sem.at[sem], recv_sem.at[sem - 3], peer(step)).start()

    def collect(ref, peers, sem, peer):
        span = ref.at[pl.ds(0, peers - 1)]
        remote(span, span, send_sem.at[sem], recv_sem.at[sem - 3], peer(1)).wait()

    low = lax.broadcasted_iota(jnp.int32, (SUB, 128), 1) < TRAIN

    def arrange(first, width, step, carry):
        begin = first + step * width
        for u in range(width):
            k = begin + u
            start = pl.multiple_of(k * EXT, 8)
            if u % 2 == 0:
                rows = pl.multiple_of(k * HALO, 2 * HALO)
                same = got_same[pl.ds(rows, 2 * HALO), :].astype(F32)
            ext_a[pl.ds(start, CH), :] = train[rng * HALF + k].astype(F32)
            ext_a[pl.ds(start + CH, HALO), :] = same[u % 2 * HALO : u % 2 * HALO + HALO]
            ext_b[pl.ds(start, CH), :] = got_train[k].astype(F32)
            ext_b[pl.ds(start + CH, HALO), :] = got_cross[k].astype(F32)[:HALO]
        for u in range(width):
            k = begin + u
            row = pl.multiple_of(k * SUB, SUB)
            for sub in range(2):
                start = k * EXT + 16 * sub + off_ref[sub]
                natural = [ext[pl.ds(start, SUB), :] for ext in (ext_a, ext_b)]
                turned = [pltpu.roll(x, 64, 1) for x in natural]
                rhs_re[sub, pl.ds(row, SUB), :] = jnp.concatenate(natural, axis=1).astype(BF16)
                rhs_im[sub, pl.ds(row, SUB), :] = jnp.concatenate([jnp.where(low, -x, x) for x in turned], axis=1).astype(
                    BF16
                )
                by_four = [
                    jnp.concatenate([ext[pl.ds(start + a, 8, stride=4), :] for a in range(4)], axis=0) * (1.0 / 128.0)
                    for ext in (ext_a, ext_b)
                ]
                lhs_cov[sub, pl.ds(row + 2 * SUB, SUB), :] = jnp.concatenate(by_four, axis=1).astype(BF16)
        return carry

    def tile(g):
        row = g * 128
        for sub in range(2):
            right = jnp.concatenate([rhs_re[sub, pl.ds(row, 128), :], rhs_im[sub, pl.ds(row, 128), :]], axis=0)
            tiles[sub, pl.ds(g * 256, 256), :] = dot_nt(lhs_cov[sub, pl.ds(row, 256), :], right)

    def pass_on(piece):
        train_copy(piece).wait_recv()

        @pl.when(core == 1)
        def _():
            relay_copy(piece).start()

    ready = [(first + count - 2) // 4 for first, count in PIECES]
    ready[-1] = HALF // 4 + 1

    def cover(piece):
        first, count = PIECES[piece]
        same_copy(piece).wait_recv()
        relay_copy(piece).wait_recv()
        width = 4 if count % 4 == 0 else 2
        lax.fori_loop(0, count // width, functools.partial(arrange, first, width), 0)
        begin = ready[piece - 1] if piece else 0
        for g in range(begin, ready[piece]):
            tile(g)
        if ready[piece] - 1 <= HEAD:
            lax.fori_loop(max(begin - 1, 0), ready[piece] - 1, functools.partial(lay_out, tiles, head, 0), 0)

    pass_on(0)
    cover(0)
    part_copy.wait()
    powers = []
    for sub in range(2):
        re = own[2 * sub] + got_part[2 * sub]
        im = own[2 * sub + 1] + got_part[2 * sub + 1]
        powers.append(re * re + im * im)
    sum_a[n_a - 1] = jnp.sum(powers[0] + powers[1], axis=0, keepdims=True)

    spread(sum_a, n_a, 7, peer_a)
    for piece in range(1, len(PIECES)):
        send_piece(piece)
    quads = [jnp.sum(p * counts, axis=1, keepdims=True) for p in powers]
    send_quad[...] = jnp.where(lane < 64, quads[0], quads[1])
    quad_copy = remote(send_quad, got_quad, send_sem.at[2], recv_sem.at[2], (chan, other))
    quad_copy.start()


    pass_on(1)

    collect(sum_a, n_a, 7, peer_a)
    sum_b[n_b - 1] = jnp.sum(sum_a[...], axis=0)
    spread(sum_b, n_b, 6, peer_b)
    cover(1)
    pass_on(2)
    cover(2)
    pass_on(3)
    cover(3)

    quad_copy.wait()
    quad_sum = send_quad[...] + got_quad[...]
    for sub in range(2):
        quad = quad_sum[:, sub * 64 : sub * 64 + 1] * (1.0 / 128.0) + norms[sub]
        matched_ref[sub] = powers[sub] / quad

    collect(sum_b, n_b, 6, peer_b)
    total = jnp.sum(jnp.sum(sum_b[...], axis=0), axis=1, keepdims=True)
    mean = total * (1.0 / (n_chan * n_rng * 2 * PULSES * GATES)) + 1e-6
    for sub in range(2):
        pmap_ref[sub] = powers[sub] / mean
    train_span, halo_span = train.at[pl.ds(0, BINS)], train_halo.at[pl.ds(0, BINS * HALO)]
    remote(train_span, got_train, send_sem.at[3], train_recv.at[0], (chan, other)).wait_send()
    remote(halo_span, got_same, send_sem.at[4], same_recv.at[0], (prev, rng)).wait_send()
    remote(train_span, got_cross, send_sem.at[5], cross_recv.at[0], (prev, rng)).wait_send()


def hand_out(tiles, head, matched, pmap, cov_out, matched_out, pmap_out, cov, sem):
    pairs = ((head, cov_out.at[pl.ds(0, HEAD * 8 * ROWS)]), (matched, matched_out), (pmap, pmap_out))
    copies = [pltpu.make_async_copy(src, dst, sem.at[i]) for i, (src, dst) in enumerate(pairs)]
    for copy in copies:
        copy.start()
    def cov_copy(g):
        source = pl.ds(pl.multiple_of((g - HEAD) * (8 * ROWS), 8 * ROWS), 8 * ROWS)
        rows = pl.ds(pl.multiple_of(g * (8 * ROWS), 8 * ROWS), 8 * ROWS)
        return pltpu.make_async_copy(cov.at[source], cov_out.at[rows], sem.at[3 + g - HEAD])

    def chunk(g, carry):
        lay_out(tiles, cov, HEAD, g, carry)
        cov_copy(g).start()
        return carry

    def chunk_done(g, carry):
        cov_copy(g).wait()
        return carry

    lax.fori_loop(HEAD, HALF // 4, chunk, 0)
    for copy in copies:
        copy.wait()
    lax.fori_loop(HEAD, HALF // 4, chunk_done, 0)


def local(sizes, radar_cube, offsets, train_index, guard_mask, weights):
    n_z, n_xy, n_chan, n_rng = sizes
    n_a, n_b = n_xy * n_rng, n_z * 2
    n_pieces = len(PIECES)
    dma = pltpu.SemaphoreType.DMA
    vmem = pl.BlockSpec(memory_space=pltpu.VMEM)
    hbm = pl.BlockSpec(memory_space=pltpu.HBM)
    rows = HALF * 2 * ROWS
    maps = (jax.ShapeDtypeStruct((2, PULSES, GATES), F32),) * 2
    held = pl.pallas_call(
        functools.partial(kernel, sizes),
        out_shape=(
            jax.ShapeDtypeStruct((2, (HALF // 4 + 1) * 256, 256), F32),
            jax.ShapeDtypeStruct((HEAD * 8 * ROWS, 128), F32),
            *maps,
        ),
        in_specs=[hbm] * 6,
        out_specs=(vmem, vmem, vmem, vmem),
        scratch_shapes=[
            pltpu.SMEM((2,), jnp.int32),
            pltpu.VMEM((2, CH, PULSES, GATES), BF16),
            pltpu.VMEM((1, TRAIN), jnp.int32),
            pltpu.VMEM((1, GATES), jnp.int32),
            pltpu.VMEM((2, 2, PULSES, 96), BF16),
            pltpu.VMEM((128, 128), BF16),
            pltpu.VMEM((2 * CH * PITCH, GATES), F32),
            pltpu.VMEM((PULSES, 2 * CH, GATES), BF16),
            pltpu.VMEM((SLOTS, CH, 128), BF16),
            pltpu.VMEM((SLOTS * HALO, 128), BF16),
            pltpu.VMEM((BINS, CH, 128), BF16),
            pltpu.VMEM((BINS * HALO, 128), BF16),
            pltpu.VMEM((BINS, CH, 128), BF16),
            pltpu.VMEM((3, PULSES // 2, 128), BF16),
            pltpu.VMEM((3, PULSES // 2, 128), BF16),
            pltpu.VMEM((PULSES * 8, 128), F32),
            pltpu.VMEM((PULSES * 8, 128), F32),
            pltpu.VMEM((PULSES * 8, 128), F32),
            pltpu.VMEM((PULSES * 8, 128), F32),
            pltpu.VMEM((4, PULSES, GATES), F32),
            pltpu.VMEM((4, PULSES, GATES), F32),
            pltpu.VMEM((PULSES, 128), F32),
            pltpu.VMEM((PULSES, 128), F32),
            pltpu.VMEM((n_a, 1, 128), F32),
            pltpu.VMEM((n_b, 1, 128), F32),
            pltpu.VMEM((BINS * EXT, 128), F32),
            pltpu.VMEM((BINS * EXT, 128), F32),
            pltpu.VMEM((2, (BINS + 2) * SUB, 256), BF16),
            pltpu.VMEM((2, (BINS + 2) * SUB, 256), BF16),
            pltpu.VMEM((2, (BINS + 6) * SUB, 256), BF16),
            dma((6,)),
            dma((8,)),
            dma((5,)),
            dma((n_pieces,)),
            dma((n_pieces,)),
            dma((n_pieces,)),
        ],
        compiler_params=pltpu.CompilerParams(
            collective_id=0, has_side_effects=True, vmem_limit_bytes=32 * 1024 * 1024
        ),
    )(
        *(
            pltpu.with_memory_space_constraint(x, pltpu.HBM)
            for x in (
                offsets,
                radar_cube,
                train_index.reshape(1, -1),
                guard_mask.reshape(1, -1),
                weights,
                jnp.asarray(dft_matrix()),
            )
        )
    )
    cov, matched, pmap = pl.pallas_call(
        hand_out,
        out_shape=(jax.ShapeDtypeStruct((rows, 128), F32), *maps),
        in_specs=[vmem] * 4,
        out_specs=(hbm, hbm, hbm),
        scratch_shapes=[pltpu.VMEM((rows - HEAD * 8 * ROWS, 128), F32), dma((3 + HALF // 4 - HEAD,))],
        compiler_params=pltpu.CompilerParams(vmem_limit_bytes=8 * 1024 * 1024),
    )(*held)
    cov = cov.reshape(HALF, 2, ROWS // 2, 2, 128).transpose(0, 1, 3, 2, 4).reshape(HALF, 2, 2, ROWS * 64)
    return cov, matched, pmap


def solution(mesh):
    n_chan, n_rng = mesh.shape["chan"], mesh.shape["rng"]
    n_xy = 8 if n_chan >= 64 else 2
    sizes = (n_chan // (2 * n_xy), n_xy, n_chan, n_rng)
    return jax.shard_map(
        functools.partial(local, sizes),
        mesh=mesh,
        in_specs=(
            P(None, "chan", None, "rng"),
            P("chan"),
            P("rng"),
            P("rng"),
            P(None, "chan", None, None),
        ),
        out_specs=(P("rng", "chan", None, None), P("chan", None, "rng"), P("chan", None, "rng")),
        check_vma=False,
    )
```

```python
import functools
import math

import jax
import jax.numpy as jnp
import numpy as np
from jax import lax
from jax.experimental import pallas as pl
from jax.experimental.pallas import tpu as pltpu
from jax.sharding import PartitionSpec as P

MESH = pl.DeviceIdType.MESH
F32 = jnp.float32
BF16 = jnp.bfloat16

PULSES = 64
CH = 32
SUB = 32
HALO = 24
EXT = CH + HALO
GATES = 128
TRAIN = 64
HALF = 32
BINS = HALF + 2
SLOTS = PULSES + 2
GROUP = 22
HEAD = 3
ROWS = 144
PITCH = PULSES + 8
PIECES = ((0, 10), (10, 8), (18, 8), (26, 8))


def dft_matrix():
    freq = np.arange(PULSES)
    angle = (freq[:, None] * freq[None, :] % PULSES) * (2.0 * math.pi / PULSES)
    cosine = np.cos(angle) / math.sqrt(PULSES)
    sine = np.sin(angle) / math.sqrt(PULSES)
    return np.block([[cosine, sine], [-sine, cosine]]).astype(jnp.bfloat16)


def dot(a, b):
    return jnp.dot(a, b, preferred_element_type=F32)


def dot_nt(a, b):
    return lax.dot_general(a, b, (((1,), (1,)), ((), ())), preferred_element_type=F32)


def turned_by(x, shift):
    return pltpu.roll(x, shift % x.shape[0], 0) if shift else x


def lay_out(tiles, cov, origin, g, carry):
    col = lax.broadcasted_iota(jnp.int32, (8, 128), 1)
    here = pl.multiple_of(g * 256, 256)
    for r in range(4):
        for sub in range(2):
            base = (((g - origin) * 4 + r) * 2 + sub) * ROWS
            for part in range(2):
                lanes = slice(part * 128, part * 128 + 128)
                by = [[], [], [], []]
                for b in range(3):
                    block = tiles[sub, pl.ds(here + (r + b + 2) * 32, 32), lanes]
                    if r >= 2:
                        after = tiles[sub, pl.ds(here + 256 + (r + b - 2) * 32, 32), lanes]
                    for a in range(4):
                        x = block[a * 8 : a * 8 + 8]
                        if r >= 2:
                            x = jnp.where(col >= r * 32, x, after[a * 8 : a * 8 + 8])
                        shift = (3 * a - r) % 4 * 32
                        by[a].append(pltpu.roll(x, shift, 1) if shift else x)
                for u, edge in enumerate((96, 64, 32)):
                    row = jnp.concatenate([jnp.where(col < edge, by[u][b], by[u + 1][b]) for b in range(3)], axis=0)
                    cov[pl.ds(base + 2 * u + part, 24, stride=6), :] = row
    return carry


def kernel(
    sizes,
    off_hbm,
    cube_hbm,
    idx_hbm,
    guard_hbm,
    wts_hbm,
    dft_hbm,
    tiles,
    head,
    matched_ref,
    pmap_ref,
    off_ref,
    cube,
    idx_ref,
    guard_ref,
    wts_ref,
    dft_ref,
    spec,
    bins,
    train,
    train_halo,
    got_train,
    got_same,
    got_cross,
    send_wts,
    got_wts,
    lhs_re,
    lhs_im,
    filt_re,
    filt_im,
    send_part,
    got_part,
    send_quad,
    got_quad,
    sum_a,
    sum_b,
    ext_a,
    ext_b,
    rhs_re,
    rhs_im,
    lhs_cov,
    fetch_sem,
    send_sem,
    recv_sem,
    train_recv,
    same_recv,
    cross_recv,
):
    n_z, n_xy, n_chan, n_rng = sizes
    n_a, n_b = n_xy * n_rng, n_z * 2
    chan, rng = lax.axis_index("chan"), lax.axis_index("rng")
    other = 1 - rng
    prev, following = lax.rem(chan + n_chan - 1, n_chan), lax.rem(chan + 1, n_chan)
    core = lax.rem(chan, 2)
    chip = chan // 2
    z, xy = chip // n_xy, lax.rem(chip, n_xy)
    my_a, my_b = xy * n_rng + rng, z * 2 + core

    def peer_a(step):
        slot = lax.rem(my_a + step, n_a)
        return (z * n_xy + slot // n_rng) * 2 + core, lax.rem(slot, n_rng)

    def peer_b(step):
        slot = lax.rem(my_b + step, n_b)
        return ((slot // 2) * n_xy + xy) * 2 + lax.rem(slot, 2), rng

    def remote(src, dst, send, recv, device):
        return pltpu.make_async_remote_copy(
            src_ref=src,
            dst_ref=dst,
            send_sem=send,
            recv_sem=recv,
            device_id=device,
            device_id_type=MESH,
        )

    fetches = [
        pltpu.make_async_copy(src, dst, fetch_sem.at[i])
        for i, (src, dst) in enumerate(
            (
                (off_hbm, off_ref),
                (wts_hbm, wts_ref),
                (idx_hbm, idx_ref),
                (guard_hbm, guard_ref),
                (dft_hbm, dft_ref),
                (cube_hbm, cube),
            )
        )
    ]
    for i in (1, 0, 5, 4):
        fetches[i].start()
    barrier = pltpu.get_barrier_semaphore()
    for device in ((prev, rng), (following, rng), (prev, other), (following, other)):
        pl.semaphore_signal(barrier, inc=1, device_id=device, device_id_type=MESH)

    for step in range(1, n_b):
        pl.semaphore_signal(barrier, inc=1, device_id=peer_b(step), device_id_type=MESH)
    for step in range(1, n_a):
        pl.semaphore_signal(barrier, inc=1, device_id=peer_a(step), device_id_type=MESH)
    for fetch in fetches[2:4]:
        fetch.start()

    fetches[0].wait()
    fetches[1].wait()
    lane = lax.broadcasted_iota(jnp.int32, (1, 128), 1)
    depth = lax.broadcasted_iota(jnp.int32, (96, 128), 0)
    placed = [[jnp.zeros((PULSES, 128), F32) for _ in range(3)] for _ in range(2)]
    group, place = lane // 32, lax.rem(lane, 32)
    for sub in range(2):
        for part in range(2):
            value = wts_ref[part, sub]
            for ahead in range(2):
                if ahead:
                    channel = CH + (place if sub else place - HALO)
                    mine = (group == part) & ((place < HALO) if sub else (place >= HALO))
                else:
                    channel = place
                    mine = group == sub * 2 + part
                at = channel - 16 * sub - off_ref[sub]
                fits = (at >= 0) & (at < SUB) & mine
                for b in range(3):
                    hot = jnp.where(depth == jnp.where(fits, at + b * SUB, -1), 1.0, 0.0).astype(BF16)
                    placed[ahead][b] = placed[ahead][b] + dot(value, hot)
    for b in range(3):
        turned = turned_by(placed[1][b], b - 1)
        send_wts[b] = (turned[:32] + pltpu.roll(turned[32:], 64, 1)).astype(BF16)

    wide = lax.broadcasted_iota(jnp.int32, (PULSES, 128), 1)

    def fill_lhs(b, sub, x):
        lhs_re[pl.ds(b * 2 + sub, PULSES, stride=8), :] = x
        lhs_im[pl.ds(b * 2 + sub, PULSES, stride=8), :] = jnp.where(
            wide < 32, -pltpu.roll(x, 96, 1), pltpu.roll(x, 32, 1)
        )

    fetches[4].wait()
    fetches[5].wait()
    table = dft_ref[...]

    def doppler(step, carry):
        for u in range(4):
            m = step * 8 + 2 * u
            pair = [jnp.concatenate([cube[0, m + v], cube[1, m + v]], axis=0) for v in range(2)]
            out = dot(table, jnp.concatenate(pair, axis=1))
            for v in range(2):
                for part in range(2):
                    start = pl.multiple_of((part * CH + m + v) * PITCH, 8)
                    spec[pl.ds(start, PULSES), :] = out[part * 64 : part * 64 + 64, v * 128 : v * 128 + 128]
        return carry

    lax.fori_loop(0, CH // 8, doppler, 0)

    pl.semaphore_wait(barrier, 4 + (n_a - 1) + (n_b - 1))
    wts_copy = remote(send_wts, got_wts, send_sem.at[0], recv_sem.at[0], (following, rng))
    wts_copy.start()

    fetches[2].wait()
    fetches[3].wait()
    gate = lax.broadcasted_iota(jnp.int32, (GATES, 128), 0)
    wanted = jnp.concatenate([idx_ref[...], idx_ref[...]], axis=1)
    hits = jnp.where(gate == wanted, 1.0, 0.0)
    guard = jnp.broadcast_to(guard_ref[...].astype(F32), (8, GATES)).astype(BF16)
    keep = dot(guard, hits.astype(BF16))[0:1]
    pick = (hits * keep).astype(BF16)
    counts = dot_nt(jnp.full((8, 128), 0.5, BF16), pick)[0:1]

    left = lax.broadcasted_iota(jnp.int32, (CH, 128), 1) < TRAIN

    def gather_bins(step):
        for u in range(GROUP):
            k = lax.rem(step * GROUP + u + PULSES - 1, PULSES)
            re = spec[pl.ds(k, CH, stride=PITCH), :]
            im = spec[pl.ds(k + CH * PITCH, CH, stride=PITCH), :]
            bins[k] = jnp.concatenate([re, im], axis=0).astype(BF16)

    def choose_gates(step):
        rows = [bins[lax.rem(step * GROUP + u + PULSES - 1, PULSES)] for u in range(GROUP)]
        chosen = dot(jnp.concatenate(rows, axis=0), pick)
        halo = []
        for u in range(GROUP):
            tile = jnp.where(left, chosen[u * 64 : u * 64 + 32], chosen[u * 64 + 32 : u * 64 + 64])
            train[step * GROUP + u] = tile.astype(BF16)
            halo.append(tile[:HALO])
        start = pl.multiple_of(step * (GROUP * HALO), GROUP * HALO)
        train_halo[pl.ds(start, GROUP * HALO), :] = jnp.concatenate(halo, axis=0).astype(BF16)

    def per_bin(step, carry):
        choose_gates(step - 1)
        gather_bins(step)
        return carry

    gather_bins(0)
    lax.fori_loop(1, SLOTS // GROUP, per_bin, 0)
    choose_gates(SLOTS // GROUP - 1)

    def train_copy(piece):
        first, count = PIECES[piece]
        return remote(
            train.at[pl.ds(other * HALF + first, count)],
            got_train.at[pl.ds(first, count)],
            send_sem.at[3],
            train_recv.at[piece],
            (chan, other),
        )

    def same_copy(piece):
        first, count = PIECES[piece]
        start = pl.multiple_of(rng * (HALF * HALO) + first * HALO, 16)
        return remote(
            train_halo.at[pl.ds(start, count * HALO)],
            got_same.at[pl.ds(first * HALO, count * HALO)],
            send_sem.at[4],
            same_recv.at[piece],
            (prev, rng),
        )

    def cross_copy(piece):
        first, count = PIECES[piece]
        return remote(
            train.at[pl.ds(other * HALF + first, count)],
            got_cross.at[pl.ds(first, count)],
            send_sem.at[5],
            cross_recv.at[piece],
            (prev, other),
        )

    def relay_copy(piece):
        first, count = PIECES[piece]
        return remote(
            got_train.at[pl.ds(first, count)],
            got_cross.at[pl.ds(first, count)],
            send_sem.at[5],
            cross_recv.at[piece],
            (prev, rng),
        )

    def send_piece(piece):
        train_copy(piece).start()

        @pl.when(core == 0)
        def _():
            same_copy(piece).start()
            cross_copy(piece).start()

    send_piece(0)

    @pl.when(core == 1)
    def _():
        for piece in range(len(PIECES)):
            same_copy(piece).start()

    def filtered():
        def one(step, carry):
            for u in range(32):
                k = step * 32 + u
                row = pl.multiple_of(k * 8, 8)
                weight = jnp.concatenate([lhs_re[pl.ds(row, 8), :], lhs_im[pl.ds(row, 8), :]], axis=0)
                out = dot(weight[:, :64].astype(BF16), bins[k])
                filt_re[pl.ds(row, 8), :] = out[:8]
                filt_im[pl.ds(row, 8), :] = out[8:]
            return carry

        lax.fori_loop(0, PULSES // 32, one, 0)
        sums = []
        for sub in range(2):
            for ref in (filt_re, filt_im):
                terms = [turned_by(ref[pl.ds(b * 2 + sub, PULSES, stride=8), :], 1 - b) for b in range(3)]
                sums.append(terms[0] + terms[1] + terms[2])
        return sums

    wts_copy.wait()
    for b in range(3):
        packed = got_wts[b].astype(F32)
        table = jnp.concatenate([packed, pltpu.roll(packed, 64, 1)], axis=0)
        fill_lhs(b, 1, jnp.where(lax.rem(wide, 32) < HALO, table, 0.0))
        fill_lhs(b, 0, jnp.where(lax.rem(wide, 32) < CH - HALO, pltpu.roll(table, 128 - HALO, 1), 0.0))
    for part, value in enumerate(filtered()):
        send_part[part] = value
    part_copy = remote(send_part, got_part, send_sem.at[1], recv_sem.at[1], (prev, rng))
    part_copy.start()

    for b in range(3):
        turned = turned_by(placed[0][b], b - 1)
        fill_lhs(b, 0, turned)
        fill_lhs(b, 1, pltpu.roll(turned, 64, 1))
    own = filtered()

    norms = []
    for sub in range(2):
        re, im = wts_ref[0, sub].astype(F32), wts_ref[1, sub].astype(F32)
        norms.append(jnp.sum(re * re + im * im, axis=1, keepdims=True))

    def spread(ref, peers, sem, peer):
        for step in range(1, peers):
            remote(ref.at[peers - 1], ref.at[step - 1], send_sem.at[sem], recv_sem.at[sem - 3], peer(step)).start()

    def collect(ref, peers, sem, peer):
        span = ref.at[pl.ds(0, peers - 1)]
        remote(span, span, send_sem.at[sem], recv_sem.at[sem - 3], peer(1)).wait()

    low = lax.broadcasted_iota(jnp.int32, (SUB, 128), 1) < TRAIN

    def arrange(first, width, step, carry):
        begin = first + step * width
        for u in range(width):
            k = begin + u
            start = pl.multiple_of(k * EXT, 8)
            if u % 2 == 0:
                rows = pl.multiple_of(k * HALO, 2 * HALO)
                same = got_same[pl.ds(rows, 2 * HALO), :].astype(F32)
            ext_a[pl.ds(start, CH), :] = train[rng * HALF + k].astype(F32)
            ext_a[pl.ds(start + CH, HALO), :] = same[u % 2 * HALO : u % 2 * HALO + HALO]
            ext_b[pl.ds(start, CH), :] = got_train[k].astype(F32)
            ext_b[pl.ds(start + CH, HALO), :] = got_cross[k].astype(F32)[:HALO]
        for u in range(width):
            k = begin + u
            row = pl.multiple_of(k * SUB, SUB)
            for sub in range(2):
                start = k * EXT + 16 * sub + off_ref[sub]
                natural = [ext[pl.ds(start, SUB), :] for ext in (ext_a, ext_b)]
                turned = [pltpu.roll(x, 64, 1) for x in natural]
                rhs_re[sub, pl.ds(row, SUB), :] = jnp.concatenate(natural, axis=1).astype(BF16)
                rhs_im[sub, pl.ds(row, SUB), :] = jnp.concatenate([jnp.where(low, -x, x) for x in turned], axis=1).astype(
                    BF16
                )
                by_four = [
                    jnp.concatenate([ext[pl.ds(start + a, 8, stride=4), :] for a in range(4)], axis=0) * (1.0 / 128.0)
                    for ext in (ext_a, ext_b)
                ]
                lhs_cov[sub, pl.ds(row + 2 * SUB, SUB), :] = jnp.concatenate(by_four, axis=1).astype(BF16)
        return carry

    def tile(g):
        row = g * 128
        for sub in range(2):
            right = jnp.concatenate([rhs_re[sub, pl.ds(row, 128), :], rhs_im[sub, pl.ds(row, 128), :]], axis=0)
            tiles[sub, pl.ds(g * 256, 256), :] = dot_nt(lhs_cov[sub, pl.ds(row, 256), :], right)

    def pass_on(piece):
        train_copy(piece).wait_recv()

        @pl.when(core == 1)
        def _():
            relay_copy(piece).start()

    ready = [(first + count - 2) // 4 for first, count in PIECES]
    ready[-1] = HALF // 4 + 1

    def cover(piece):
        first, count = PIECES[piece]
        same_copy(piece).wait_recv()
        relay_copy(piece).wait_recv()
        width = 4 if count % 4 == 0 else 2
        lax.fori_loop(0, count // width, functools.partial(arrange, first, width), 0)
        begin = ready[piece - 1] if piece else 0
        for g in range(begin, ready[piece]):
            tile(g)
        if ready[piece] - 1 <= HEAD:
            lax.fori_loop(max(begin - 1, 0), ready[piece] - 1, functools.partial(lay_out, tiles, head, 0), 0)

    @pl.when(core == 1)
    def _():
        pass_on(0)
        cover(0)

    part_copy.wait()
    powers = []
    for sub in range(2):
        re = own[2 * sub] + got_part[2 * sub]
        im = own[2 * sub + 1] + got_part[2 * sub + 1]
        powers.append(re * re + im * im)
    sum_a[n_a - 1] = jnp.sum(powers[0] + powers[1], axis=0, keepdims=True)

    spread(sum_a, n_a, 7, peer_a)

    @pl.when(core == 0)
    def _():
        pass_on(0)
        cover(0)

    for piece in range(1, len(PIECES)):
        send_piece(piece)
    quads = [jnp.sum(p * counts, axis=1, keepdims=True) for p in powers]
    send_quad[...] = jnp.where(lane < 64, quads[0], quads[1])
    quad_copy = remote(send_quad, got_quad, send_sem.at[2], recv_sem.at[2], (chan, other))
    quad_copy.start()


    pass_on(1)

    collect(sum_a, n_a, 7, peer_a)
    sum_b[n_b - 1] = jnp.sum(sum_a[...], axis=0)
    spread(sum_b, n_b, 6, peer_b)
    cover(1)
    pass_on(2)
    cover(2)
    pass_on(3)
    cover(3)

    quad_copy.wait()
    quad_sum = send_quad[...] + got_quad[...]
    for sub in range(2):
        quad = quad_sum[:, sub * 64 : sub * 64 + 1] * (1.0 / 128.0) + norms[sub]
        matched_ref[sub] = powers[sub] / quad

    collect(sum_b, n_b, 6, peer_b)
    total = jnp.sum(jnp.sum(sum_b[...], axis=0), axis=1, keepdims=True)
    mean = total * (1.0 / (n_chan * n_rng * 2 * PULSES * GATES)) + 1e-6
    for sub in range(2):
        pmap_ref[sub] = powers[sub] / mean
    train_span, halo_span = train.at[pl.ds(0, BINS)], train_halo.at[pl.ds(0, BINS * HALO)]
    remote(train_span, got_train, send_sem.at[3], train_recv.at[0], (chan, other)).wait_send()
    remote(halo_span, got_same, send_sem.at[4], same_recv.at[0], (prev, rng)).wait_send()
    remote(train_span, got_cross, send_sem.at[5], cross_recv.at[0], (prev, rng)).wait_send()


def hand_out(tiles, head, matched, pmap, cov_out, matched_out, pmap_out, cov, sem):
    pairs = ((head, cov_out.at[pl.ds(0, HEAD * 8 * ROWS)]), (matched, matched_out), (pmap, pmap_out))
    copies = [pltpu.make_async_copy(src, dst, sem.at[i]) for i, (src, dst) in enumerate(pairs)]
    for copy in copies:
        copy.start()
    def cov_copy(g):
        source = pl.ds(pl.multiple_of((g - HEAD) * (8 * ROWS), 8 * ROWS), 8 * ROWS)
        rows = pl.ds(pl.multiple_of(g * (8 * ROWS), 8 * ROWS), 8 * ROWS)
        return pltpu.make_async_copy(cov.at[source], cov_out.at[rows], sem.at[3 + g - HEAD])

    def chunk(g, carry):
        lay_out(tiles, cov, HEAD, g, carry)
        cov_copy(g).start()
        return carry

    def chunk_done(g, carry):
        cov_copy(g).wait()
        return carry

    lax.fori_loop(HEAD, HALF // 4, chunk, 0)
    for copy in copies:
        copy.wait()
    lax.fori_loop(HEAD, HALF // 4, chunk_done, 0)


def local(sizes, radar_cube, offsets, train_index, guard_mask, weights):
    n_z, n_xy, n_chan, n_rng = sizes
    n_a, n_b = n_xy * n_rng, n_z * 2
    n_pieces = len(PIECES)
    dma = pltpu.SemaphoreType.DMA
    vmem = pl.BlockSpec(memory_space=pltpu.VMEM)
    hbm = pl.BlockSpec(memory_space=pltpu.HBM)
    rows = HALF * 2 * ROWS
    maps = (jax.ShapeDtypeStruct((2, PULSES, GATES), F32),) * 2
    held = pl.pallas_call(
        functools.partial(kernel, sizes),
        out_shape=(
            jax.ShapeDtypeStruct((2, (HALF // 4 + 1) * 256, 256), F32),
            jax.ShapeDtypeStruct((HEAD * 8 * ROWS, 128), F32),
            *maps,
        ),
        in_specs=[hbm] * 6,
        out_specs=(vmem, vmem, vmem, vmem),
        scratch_shapes=[
            pltpu.SMEM((2,), jnp.int32),
            pltpu.VMEM((2, CH, PULSES, GATES), BF16),
            pltpu.VMEM((1, TRAIN), jnp.int32),
            pltpu.VMEM((1, GATES), jnp.int32),
            pltpu.VMEM((2, 2, PULSES, 96), BF16),
            pltpu.VMEM((128, 128), BF16),
            pltpu.VMEM((2 * CH * PITCH, GATES), F32),
            pltpu.VMEM((PULSES, 2 * CH, GATES), BF16),
            pltpu.VMEM((SLOTS, CH, 128), BF16),
            pltpu.VMEM((SLOTS * HALO, 128), BF16),
            pltpu.VMEM((BINS, CH, 128), BF16),
            pltpu.VMEM((BINS * HALO, 128), BF16),
            pltpu.VMEM((BINS, CH, 128), BF16),
            pltpu.VMEM((3, PULSES // 2, 128), BF16),
            pltpu.VMEM((3, PULSES // 2, 128), BF16),
            pltpu.VMEM((PULSES * 8, 128), F32),
            pltpu.VMEM((PULSES * 8, 128), F32),
            pltpu.VMEM((PULSES * 8, 128), F32),
            pltpu.VMEM((PULSES * 8, 128), F32),
            pltpu.VMEM((4, PULSES, GATES), F32),
            pltpu.VMEM((4, PULSES, GATES), F32),
            pltpu.VMEM((PULSES, 128), F32),
            pltpu.VMEM((PULSES, 128), F32),
            pltpu.VMEM((n_a, 1, 128), F32),
            pltpu.VMEM((n_b, 1, 128), F32),
            pltpu.VMEM((BINS * EXT, 128), F32),
            pltpu.VMEM((BINS * EXT, 128), F32),
            pltpu.VMEM((2, (BINS + 2) * SUB, 256), BF16),
            pltpu.VMEM((2, (BINS + 2) * SUB, 256), BF16),
            pltpu.VMEM((2, (BINS + 6) * SUB, 256), BF16),
            dma((6,)),
            dma((8,)),
            dma((5,)),
            dma((n_pieces,)),
            dma((n_pieces,)),
            dma((n_pieces,)),
        ],
        compiler_params=pltpu.CompilerParams(
            collective_id=0, has_side_effects=True, vmem_limit_bytes=32 * 1024 * 1024
        ),
    )(
        *(
            pltpu.with_memory_space_constraint(x, pltpu.HBM)
            for x in (
                offsets,
                radar_cube,
                train_index.reshape(1, -1),
                guard_mask.reshape(1, -1),
                weights,
                jnp.asarray(dft_matrix()),
            )
        )
    )
    cov, matched, pmap = pl.pallas_call(
        hand_out,
        out_shape=(jax.ShapeDtypeStruct((rows, 128), F32), *maps),
        in_specs=[vmem] * 4,
        out_specs=(hbm, hbm, hbm),
        scratch_shapes=[pltpu.VMEM((rows - HEAD * 8 * ROWS, 128), F32), dma((3 + HALF // 4 - HEAD,))],
        compiler_params=pltpu.CompilerParams(vmem_limit_bytes=8 * 1024 * 1024),
    )(*held)
    cov = cov.reshape(HALF, 2, ROWS // 2, 2, 128).transpose(0, 1, 3, 2, 4).reshape(HALF, 2, 2, ROWS * 64)
    return cov, matched, pmap


def solution(mesh):
    n_chan, n_rng = mesh.shape["chan"], mesh.shape["rng"]
    n_xy = 8 if n_chan >= 64 else 2
    sizes = (n_chan // (2 * n_xy), n_xy, n_chan, n_rng)
    return jax.shard_map(
        functools.partial(local, sizes),
        mesh=mesh,
        in_specs=(
            P(None, "chan", None, "rng"),
            P("chan"),
            P("rng"),
            P("rng"),
            P(None, "chan", None, None),
        ),
        out_specs=(P("rng", "chan", None, None), P("chan", None, "rng"), P("chan", None, "rng")),
        check_vma=False,
    )
```
